512 devices in a mesh: panel: 32 (over y_lo, z, core), rhs: 16 (over x, y_hi).
Axes of the slice: x: 4, y: 8 (y_hi: 4, y_lo: 2; y = y_hi * 2 + y_lo), z: 8, core: 2. Of those that a mesh axis runs over, the one named last changes fastest.
Arguments:
- pivot_rhs: float32 [2, 2048, 2048], P(None, 'panel', 'rhs'), may hold values from -6 to 6
- update_rhs: float32 [4096, 2048], P('panel', 'rhs'), may hold values from -6 to 6
- parent_rhs: float32 [4096, 2048], P('panel', 'rhs'), may hold values from -6 to 6
- lower_pivot: bfloat16 [2, 2048, 2048], P(None, 'panel', 'rhs'), may hold values from -1 to 1.4, as said below
- lower_update: bfloat16 [4096, 2048], P('panel', 'rhs'), may hold values from -0.125 to 0.125
- parent_lower: bfloat16 [4096, 4096], P('panel', 'rhs'), may hold values from -1 to 1.4, as said below
- parent_upper: bfloat16 [4096, 4096], P('panel', 'rhs'), may hold values from -1 to 1.4, as said below
- upper_pivot: bfloat16 [2, 2048, 2048], P(None, 'panel', 'rhs'), may hold values from -1 to 1.4, as said below
- upper_update: bfloat16 [2, 2048, 2048], P(None, 'panel', 'rhs'), may hold values from -0.125 to 0.125
- maps: int32 [4096], replicated, may hold values from 0 to 4095, as said below
Outputs:
- parent_solution: float32 [4096, 2048], P('panel', 'rhs')
- child_solution: float32 [2, 2048, 2048], P(None, 'panel', 'rhs')
The draws below stay inside these ranges and needn't reach their ends.
Inputs may be any that keep to these rules, and one draw needn't show every extreme that they name: `maps`: for each child k, entry k * 2048 + i is 2 * i + b with b equal to 0 or 1; both values of b occur for each child in every draw. `lower_pivot`: each block is lower triangular, diagonal 0.6 to 1.4. `upper_pivot`: each block is upper triangular, diagonal 0.6 to 1.4. `parent_lower`: lower triangular, diagonal 0.6 to 1.4. `parent_upper`: upper triangular, diagonal 0.6 to 1.4.
All inputs are finite; a program needn't handle non-finite values.
Results may differ from the reference program's by a relative error of at most 0.0054.
Values may be sent and summed in bfloat16 or wider, within the bound.
A program may use at most 64 MiB of HBM per device.

```python
import math
import jax
import jax.numpy as jnp
from jax import lax

F = 4096
KC = 2048
FU = 2048
RHS = 2048


def triangle(random_key, block_count, matrix_order, lower_side):
    shape_full = (block_count, matrix_order, matrix_order)
    noise = jax.random.normal(random_key, shape_full, jnp.float32)
    noise = noise / math.sqrt(matrix_order)
    row_ids = lax.broadcasted_iota(jnp.int32, (matrix_order, matrix_order), 0)
    col_ids = lax.broadcasted_iota(jnp.int32, (matrix_order, matrix_order), 1)
    if lower_side:
        keeper = row_ids > col_ids
    else:
        keeper = row_ids < col_ids
    diagonal_scale = jax.random.uniform(jax.random.fold_in(random_key, 7), (block_count, matrix_order, 1), jnp.float32, 0.6, 1.4)
    identity = jnp.where(row_ids == col_ids, 1.0, 0.0).astype(jnp.float32)
    return jnp.where(keeper[None], noise, 0.0) + identity[None] * diagonal_scale


def draw_lower_pivot(key, part):
    return triangle(jax.random.fold_in(key, 101), 2, KC, True).astype(jnp.bfloat16)


def draw_upper_pivot(key, part):
    return triangle(jax.random.fold_in(key, 103), 2, KC, False).astype(jnp.bfloat16)


def draw_parent_lower(key, part):
    return triangle(jax.random.fold_in(key, 107), 1, F, True).reshape(F, F).astype(jnp.bfloat16)


def draw_parent_upper(key, part):
    return triangle(jax.random.fold_in(key, 109), 1, F, False).reshape(F, F).astype(jnp.bfloat16)


def draw_maps(key, part):
    local = lax.broadcasted_iota(jnp.int32, (FU,), 0)
    first_bits = jax.random.randint(jax.random.fold_in(key, 211), (FU,), 0, 2)
    first_bits = jnp.where(local == 0, 0, first_bits)
    first_bits = jnp.where(local == FU - 1, 1, first_bits)
    second_bits = jax.random.randint(jax.random.fold_in(key, 212), (FU,), 0, 2)
    second_bits = jnp.where(local == 0, 1, second_bits)
    second_bits = jnp.where(local == FU - 1, 0, second_bits)
    return jnp.concatenate([2 * local + first_bits, 2 * local + second_bits]).astype(jnp.int32)


def levels(key, dims, shards, smallest, top_value):
    factor_of, own = 1.0, jax.random.fold_in(key, 6)
    for axis_at, blocks in shards:
        draws = jnp.exp(jax.random.uniform(jax.random.fold_in(own, axis_at), (blocks,), jnp.float32, smallest / len(shards), top_value / len(shards)))
        factor_of = factor_of * jnp.repeat(draws, dims[axis_at] // blocks).reshape([-1 if axis == axis_at else 1 for axis in range(len(dims))])
    return factor_of


def normal_values(stream_key, extent, spread, bound, pieces=(), held_as=jnp.bfloat16):
    level = levels(stream_key, extent, pieces, -0.22, 0.18) if pieces else 1.0
    drawn = jax.random.normal(stream_key, extent, jnp.float32) * spread * level
    return jnp.minimum(jnp.maximum(drawn, -bound), bound).astype(held_as)


def setup_inputs(seed: int = 0) -> dict:
    key_of = jax.random.split(jax.random.key(seed), 11)
    return {
        "pivot_rhs": normal_values(key_of[0], (2, KC, RHS), 1.0, 6.0, ((1, 32), (2, 16)), jnp.float32),
        "update_rhs": normal_values(key_of[1], (2 * FU, RHS), 1.0, 6.0, ((0, 32), (1, 16)), jnp.float32),
        "parent_rhs": normal_values(key_of[2], (F, RHS), 1.0, 6.0, ((0, 32), (1, 16)), jnp.float32),
        "lower_pivot": draw_lower_pivot(jax.random.fold_in(key_of[10], 71), 0),
        "lower_update": normal_values(key_of[4], (2 * FU, KC), KC ** -0.5, 0.125, ((0, 32), (1, 16))),
        "parent_lower": draw_parent_lower(jax.random.fold_in(key_of[10], 71), 0),
        "parent_upper": draw_parent_upper(jax.random.fold_in(key_of[10], 71), 0),
        "upper_pivot": draw_upper_pivot(jax.random.fold_in(key_of[10], 71), 0),
        "upper_update": normal_values(key_of[8], (2, KC, FU), FU ** -0.5, 0.125, ((1, 32), (2, 16))),
        "maps": draw_maps(jax.random.fold_in(key_of[10], 71), 0),
    }


def product(left, right):
    return jnp.dot(left, right, preferred_element_type=jnp.float32)


def reference(pivot_rhs, update_rhs, parent_rhs, lower_pivot, lower_update, parent_lower, parent_upper, upper_pivot, upper_update, maps):
    pivot_input = pivot_rhs.astype(jnp.bfloat16)
    solved = []
    updates = []
    for member in range(2):
        source = pivot_input[member]
        solved.append(product(lower_pivot[member], source))
        updates.append(update_rhs[member * FU:(member + 1) * FU] + product(lower_update[member * FU:(member + 1) * FU], source))
    pivot_half = jnp.stack(solved, axis=0).astype(jnp.bfloat16)
    update_half = jnp.concatenate(updates, axis=0).astype(jnp.bfloat16)
    widened = lax.optimization_barrier(update_half).astype(jnp.float32)
    scattered = jnp.zeros(parent_rhs.shape, jnp.float32).at[maps].add(widened)
    parent_sum = parent_rhs + scattered
    parent_mid = product(parent_lower, parent_sum.astype(jnp.bfloat16))
    parent_solution = product(parent_upper, parent_mid.astype(jnp.bfloat16))
    solution_half = parent_solution.astype(jnp.bfloat16)
    blocks = []
    for member in range(2):
        picked = jnp.take(solution_half, maps[member * FU:(member + 1) * FU], axis=0)
        direct = product(upper_pivot[member], pivot_half[member])
        blocks.append(direct + product(upper_update[member], picked))
    return parent_solution, jnp.stack(blocks, axis=0)
```

```python
import functools

import jax
import jax.numpy as jnp
from jax import lax
from jax.experimental import pallas as pl
from jax.experimental.pallas import tpu as pltpu
from jax.sharding import PartitionSpec as P

BF = jnp.bfloat16
F32 = jnp.float32
MESH = pl.DeviceIdType.MESH

Z = 8
DIST = (0, -1, 1, -2, 2, -3, 3, 4)
N_GATHER, N_SPREAD = 5, 4
SENDS = 32


def dot(left, right):
    return jnp.dot(left, right, preferred_element_type=F32)


def kernel(
    pivot_rhs,
    update_rhs,
    parent_rhs,
    lower_pivot,
    lower_update,
    parent_lower,
    parent_upper,
    upper_pivot,
    upper_update,
    maps,
    parent_out,
    child_out,
    x_pin,
    x_half,
    x_sol,
    x_sum,
    x_mid,
    a_low,
    a_par,
    a_piv,
    a_up,
    moved_rhs,
    pick,
    acc,
    direct,
    g_send,
    g_recv,
    s_send,
    s_recv,
    e_send,
    e_recv,
    h_send,
    h_recv,
):
    me_p, me_r = lax.axis_index("panel"), lax.axis_index("rhs")
    core = lax.rem(me_p, 2)
    c = me_p // 2
    z, y_lo = lax.rem(c, Z), c // Z
    x, y_hi = me_r // 4, lax.rem(me_r, 4)
    mate_y = 1 - y_lo
    sib = me_p + 1 - 2 * core

    def chip(y, dist):
        return y * Z + lax.rem(z + dist + Z, Z)

    def at_z(dist):
        return chip(y_lo, dist) * 2 + core

    def at_xy(dx, dy):
        return lax.rem(x + dx + 4, 4) * 4 + lax.rem(y_hi + dy + 4, 4)

    across = (mate_y * Z + z) * 2 + core
    goal = lax.rem(me_p, 2 * Z) * 2

    barrier = pltpu.get_barrier_semaphore()
    friends = [(at_z(d), me_r) for d in (-1, 1, -2, 2)] + [(across, me_r), (sib, me_r)]
    friends += [(me_p, at_xy(*d)) for d in ((0, -1), (0, 1), (-1, 0), (1, 0))]
    for friend in friends:
        pl.semaphore_signal(barrier, inc=1, device_id=friend, device_id_type=MESH)
    for child in range(2):
        source = c + 2 * Z * child

        @pl.when(source != me_p)
        def _():
            pl.semaphore_signal(barrier, inc=1, device_id=(source, me_r), device_id_type=MESH)

    pending = []

    def rcopy(src, dst, send, recv, device):
        return pltpu.make_async_remote_copy(
            src_ref=src, dst_ref=dst, send_sem=send, recv_sem=recv, device_id=device, device_id_type=MESH
        )

    def send(src, dst, ssem, rsem, device, when=None):
        def go():
            rcopy(src, dst, ssem, rsem, device).start()

        def done():
            rcopy(src, dst, ssem, rsem, device).wait_send()

        pending.append((when, done))
        if when is None:
            go()
        else:
            pl.when(when)(go)

    def landed(ref, sem):
        pltpu.make_async_copy(ref, ref, sem).wait()

    class Gather:
        def __init__(self, g, place):
            self.g, self.place, self.n = g, place, 0

        def sem(self, side, col, dist):
            return g_recv.at[self.g, side * 16 + col * 8 + DIST.index(dist)]

        def block(self, col, dist, side=0):
            y = y_lo if col == 0 else mate_y
            return self.place(chip(y, dist), core if side == 0 else 1 - core)

        def put(self, col, dist, to, side, col_there, dist_there, when=None):
            ref = self.block(col, dist)
            send(
                ref,
                ref,
                g_send.at[self.g, self.n],
                self.sem(side, col_there, dist_there),
                (to, me_r),
                when,
            )
            self.n += 1

        def start(self):
            for d in (2, -2, 1, -1):
                self.put(0, 0, at_z(d), 0, 0, -d)
            self.put(0, 0, across, 0, 1, 0)
            self.put(0, 0, sib, 1, 0, 0)

        def hop(self, d):
            landed(self.block(0, d), self.sem(0, 0, d))
            if d == -2:
                self.put(0, d, at_z(1), 0, 0, -3)
                self.put(0, d, at_z(2), 0, 0, 4, core == 0)
            if d == 2:
                self.put(0, d, at_z(-1), 0, 0, 3)
                self.put(0, d, at_z(-2), 0, 0, 4, core == 1)
            self.put(0, d, across, 0, 1, d)
            self.put(0, d, sib, 1, 0, d)

        def over(self, d):
            landed(self.block(1, d), self.sem(0, 1, d))
            self.put(1, d, sib, 1, 1, d)

        def arrive(self, col, d):
            landed(self.block(col, d, 1), self.sem(1, col, d))

    class Spread:
        def __init__(self, a, place):
            self.a, self.place, self.n = a, place, 0

        def sem(self, hop, piece):
            return s_recv.at[self.a, hop * 4 + piece]

        def block(self, hop, piece):
            dx = {0: 0, 1: -1, 2: 1, 3: 2}[hop]
            dy = {0: 0, 1: -1, 2: 1, 3: 2}[piece]
            return self.place(at_xy(dx, dy))

        def put(self, hop, piece, to, hop_there, piece_there, when=None):
            ref = self.block(hop, piece)
            send(
                ref,
                ref,
                s_send.at[self.a, self.n],
                self.sem(hop_there, piece_there),
                (me_p, to),
                when,
            )
            self.n += 1

        def start(self):
            self.put(0, 0, at_xy(0, 1), 0, 1)
            self.put(0, 0, at_xy(0, -1), 0, 2)

        def wait(self, hop, piece):
            landed(self.block(hop, piece), self.sem(hop, piece))

        def turn(self):
            self.wait(0, 1)
            self.put(0, 1, at_xy(0, 1), 0, 3, core == 0)
            self.wait(0, 2)
            self.put(0, 2, at_xy(0, -1), 0, 3, core == 1)

        def out(self, piece):
            if piece == 3:
                self.wait(0, 3)
            self.put(0, piece, at_xy(1, 0), 1, piece)
            self.put(0, piece, at_xy(-1, 0), 2, piece)

        def on(self, piece):
            self.wait(1, piece)
            self.put(1, piece, at_xy(1, 0), 3, piece, core == 0)
            self.wait(2, piece)
            self.put(2, piece, at_xy(-1, 0), 3, piece, core == 1)

        def end(self):
            for piece in range(4):
                self.wait(3, piece)

    class Extra:
        def __init__(self, e, ref):
            self.e, self.ref = e, ref
            self.dx = lax.rem(x - c // 4 + 4, 4)
            self.dy = lax.rem(y_hi - lax.rem(c, 4) + 4, 4)
            self.n = 0

        def put(self, to, when):
            send(self.ref, self.ref, e_send.at[self.e, self.n], e_recv.at[self.e], (me_p, to), when)
            self.n += 1

        def wait(self, when):
            @pl.when(when)
            def _():
                landed(self.ref, e_recv.at[self.e])

        def both(self, *conditions):
            return functools.reduce(jnp.logical_and, conditions)

        def start(self):
            source = self.both(self.dx == 0, self.dy == 0)
            self.put(at_xy(0, 1), source)
            self.put(at_xy(0, -1), source)
            self.put(at_xy(1, 0), source)
            self.put(at_xy(-1, 0), source)

        def turn(self):
            low, high = self.both(self.dx == 0, self.dy == 1), self.both(self.dx == 0, self.dy == 3)
            near = self.both(self.dx == 0, lax.rem(self.dy, 2) == 1)
            self.wait(near)
            self.put(at_xy(0, 1), self.both(low, core == 0))
            self.put(at_xy(0, -1), self.both(high, core == 1))
            self.put(at_xy(1, 0), near)
            self.put(at_xy(-1, 0), near)

        def out(self):
            far = self.both(self.dx == 0, self.dy == 2)
            self.wait(far)
            self.put(at_xy(1, 0), far)
            self.put(at_xy(-1, 0), far)

        def on(self):
            self.wait(lax.rem(self.dx, 2) == 1)
            self.put(at_xy(1, 0), self.both(self.dx == 1, core == 0))
            self.put(at_xy(-1, 0), self.both(self.dx == 3, core == 1))

        def end(self):
            self.wait(self.dx == 2)

    def two(buffer):
        return lambda chip_at, core_at: buffer.at[:, chip_at, core_at]

    def one(buffer):
        return lambda chip_at, core_at: buffer.at[chip_at, core_at]

    def slot(r):
        return r + (r + 15 - c) // 16

    g_pin = Gather(0, two(x_pin))
    g_sum = Gather(1, one(x_sum))
    g_mid = Gather(2, one(x_mid))
    g_sol = Gather(3, two(x_sol))
    g_half = Gather(4, two(x_half))
    f_low = Spread(0, lambda r: a_low.at[r])
    f_par = Spread(1, lambda r: a_par.at[slot(r)])
    f_piv = Spread(2, lambda r: a_piv.at[slot(r)])
    f_up = Spread(3, lambda r: a_up.at[r])
    e_par = Extra(0, a_par.at[c + 1])
    e_piv = Extra(1, a_piv.at[c + 1])

    x_pin[:, c, core] = pivot_rhs[...].astype(BF)

    @pl.when(me_r <= c)
    def _():
        a_par[me_r] = parent_lower[...]
        a_piv[me_r] = lower_pivot[...]

    @pl.when(me_r >= c)
    def _():
        a_par[me_r + 1] = parent_upper[...]
        a_piv[me_r + 1] = upper_pivot[...]

    a_up[me_r] = upper_update[...]
    alone = (31 - me_p) // 31 + me_p // 31
    pl.semaphore_wait(barrier, len(friends) + 2 - alone)

    def shuffle(src, dst, n):
        for side in range(2):
            there = goal + side
            piece = src.at[pl.ds(side * 64, 64)]
            send(piece, dst, h_send.at[n, side], h_recv.at[n, y_lo], (there, me_r), there != me_p)

            @pl.when(there == me_p)
            def _():
                pltpu.make_async_copy(piece, dst, h_recv.at[n, y_lo]).start()

    shuffle(lower_update, a_low.at[me_r, y_lo], 0)
    g_pin.start()
    f_par.start()
    f_par.out(0)
    shuffle(update_rhs, moved_rhs.at[y_lo], 1)

    start = pl.multiple_of(c * 128, 128)
    lanes = [maps[:, pl.ds(k * 2048 + start, 128)] - me_p * 128 for k in range(2)]
    low = jnp.concatenate([lanes[0][:, :64], lanes[1][:, :64]], axis=1)
    high = jnp.concatenate([lanes[0][:, 64:], lanes[1][:, 64:]], axis=1)
    targets = jnp.where(core == 0, low, high)
    rows = lax.broadcasted_iota(jnp.int32, (128, 128), 0)
    chosen = (rows == targets).astype(F32)
    pick[0] = chosen.astype(BF)
    pick[1] = chosen.T.astype(BF)

    g_pin.hop(-2)
    g_pin.hop(2)
    g_pin.hop(-1)
    g_pin.hop(1)
    g_pin.over(0)
    for child in range(2):
        landed(a_low.at[me_r, child], h_recv.at[0, child])
    f_low.start()
    f_low.out(0)
    g_pin.over(-1)
    g_pin.over(1)
    for d in (-3, 3, 4):
        g_pin.hop(d)
    f_par.turn()
    f_par.out(1)
    f_par.out(2)
    f_low.turn()
    f_low.out(1)
    f_low.out(2)
    for d in (-2, 2, -3, 3, 4):
        g_pin.over(d)
    f_low.out(3)
    for piece in (0, 1, 2):
        f_low.on(piece)
    f_low.on(3)
    f_par.out(3)
    e_par.start()
    e_piv.start()
    for child in range(2):
        landed(moved_rhs.at[child], h_recv.at[1, child])
    for col in range(2):
        for d in DIST:
            g_pin.arrive(col, d)
    f_low.end()

    def blocks(buffer, k, r):
        return buffer[k, r].reshape(128, 128)

    halves = []
    for k in range(2):
        value = moved_rhs[k]
        for r in range(16):
            value += dot(a_low[r, k], blocks(x_pin, k, r))
        halves.append(value.astype(BF))
    total = parent_rhs[...] + dot(pick[0], jnp.concatenate(halves, axis=0))
    x_sum[c, core] = total.astype(BF)
    g_sum.start()

    f_piv.start()
    f_piv.out(0)
    f_up.start()
    f_par.on(0)
    g_sum.hop(-2)
    g_sum.hop(2)
    g_sum.hop(-1)
    g_sum.hop(1)
    f_par.on(1)
    f_par.on(2)
    g_sum.over(0)
    g_sum.over(-1)
    g_sum.over(1)
    for d in (-3, 3, 4):
        g_sum.hop(d)
    f_par.on(3)
    e_par.turn()
    for d in (-2, 2, -3, 3, 4):
        g_sum.over(d)
    f_par.end()
    for col in range(2):
        for d in DIST:
            g_sum.arrive(col, d)

    def pair(buffer, r):
        return buffer[r].reshape(256, 128)

    def lower(r):
        return r <= c

    def upper(r):
        return r >= c

    acc[...] = jnp.zeros_like(acc)
    for r in range(16):

        @pl.when(lower(r))
        def _():
            acc[...] += dot(a_par[r], pair(x_sum, r))

    x_mid[c, core] = acc[...].astype(BF)
    g_mid.start()

    f_piv.turn()
    f_piv.out(1)
    f_piv.out(2)
    f_up.out(0)
    g_mid.hop(-2)
    g_mid.hop(2)
    g_mid.hop(-1)
    g_mid.hop(1)
    f_up.turn()
    f_piv.out(3)
    e_par.out()
    e_piv.turn()
    g_mid.over(0)
    g_mid.over(-1)
    g_mid.over(1)
    for d in (-3, 3, 4):
        g_mid.hop(d)
    f_up.out(1)
    f_up.out(2)
    f_up.out(3)
    for piece in range(4):
        f_piv.on(piece)
    e_par.on()
    e_piv.out()
    for d in (-2, 2, -3, 3, 4):
        g_mid.over(d)
    f_piv.end()
    e_piv.on()

    direct[...] = jnp.zeros_like(direct)
    for r in range(16):

        @pl.when(lower(r))
        def _():
            for k in range(2):
                direct[k] += dot(a_piv[r, k], blocks(x_pin, k, r))

    x_half[:, c, core] = direct[...].astype(BF)
    g_half.start()
    for col in range(2):
        for d in DIST:
            g_mid.arrive(col, d)
    e_par.end()

    acc[...] = jnp.zeros_like(acc)
    for r in range(16):

        @pl.when(upper(r))
        def _():
            acc[...] += dot(a_par[r + 1], pair(x_mid, r))

    parent_out[...] = acc[...]
    picked = dot(pick[1], acc[...].astype(BF)).astype(BF)
    x_sol[:, c, core] = picked.reshape(2, 64, 128)
    g_sol.start()

    for d in (-2, 2, -1, 1):
        g_half.hop(d)
    g_half.over(0)
    for piece in range(4):
        f_up.on(piece)
    for d in (-2, 2, -1, 1):
        g_sol.hop(d)
    g_sol.over(0)
    g_sol.over(-1)
    g_sol.over(1)
    for d in (-3, 3, 4):
        g_half.hop(d)
    for d in (-3, 3, 4):
        g_sol.hop(d)
    for d in (-1, 1, -2, 2, -3, 3, 4):
        g_half.over(d)
    for d in (-2, 2, -3, 3, 4):
        g_sol.over(d)
    e_piv.end()
    for col in range(2):
        for d in DIST:
            g_half.arrive(col, d)

    direct[...] = jnp.zeros_like(direct)
    for r in range(16):

        @pl.when(upper(r))
        def _():
            for k in range(2):
                direct[k] += dot(a_piv[r + 1, k], blocks(x_half, k, r))

    f_up.end()
    for col in range(2):
        for d in DIST:
            g_sol.arrive(col, d)
    for k in range(2):
        value = direct[k]
        for r in range(16):
            value += dot(a_up[r, k], blocks(x_sol, k, r))
        child_out[k] = value

    for when, done in pending:
        if when is None:
            done()
        else:
            pl.when(when)(done)


def shards(*arguments):
    *arrays, maps = arguments
    vm = pltpu.VMEM
    dma = pltpu.SemaphoreType.DMA
    return pl.pallas_call(
        kernel,
        out_shape=(
            jax.ShapeDtypeStruct((128, 128), F32),
            jax.ShapeDtypeStruct((2, 64, 128), F32),
        ),
        in_specs=[pl.BlockSpec(memory_space=pltpu.VMEM)] * 10,
        out_specs=(pl.BlockSpec(memory_space=pltpu.VMEM),) * 2,
        scratch_shapes=[
            vm((2, 16, 2, 64, 128), BF),
            vm((2, 16, 2, 64, 128), BF),
            vm((2, 16, 2, 64, 128), BF),
            vm((16, 2, 128, 128), BF),
            vm((16, 2, 128, 128), BF),
            vm((16, 2, 64, 128), BF),
            vm((17, 128, 256), BF),
            vm((17, 2, 64, 128), BF),
            vm((16, 2, 64, 128), BF),
            vm((2, 64, 128), F32),
            vm((2, 128, 128), BF),
            vm((128, 128), F32),
            vm((2, 64, 128), F32),
            dma((N_GATHER, SENDS)),
            dma((N_GATHER, 32)),
            dma((N_SPREAD, 20)),
            dma((N_SPREAD, 16)),
            dma((2, 12)),
            dma((2,)),
            dma((2, 2)),
            dma((2, 2)),
        ],
        compiler_params=pltpu.CompilerParams(
            collective_id=0, has_side_effects=True, vmem_limit_bytes=60 * 1024 * 1024
        ),
    )(*arrays, maps.reshape(1, -1))


def solution(mesh):
    placed = (
        P(None, "panel", "rhs"),
        P("panel", "rhs"),
        P("panel", "rhs"),
        P(None, "panel", "rhs"),
        P("panel", "rhs"),
        P("panel", "rhs"),
        P("panel", "rhs"),
        P(None, "panel", "rhs"),
        P(None, "panel", "rhs"),
        P(),
    )
    return jax.shard_map(
        shards,
        mesh=mesh,
        in_specs=placed,
        out_specs=(P("panel", "rhs"), P(None, "panel", "rhs")),
        check_vma=False,
    )
```

```python
import functools

import jax
import jax.numpy as jnp
from jax import lax
from jax.experimental import pallas as pl
from jax.experimental.pallas import tpu as pltpu
from jax.sharding import PartitionSpec as P

BF = jnp.bfloat16
F32 = jnp.float32
MESH = pl.DeviceIdType.MESH

Z = 8
DIST = (0, -1, 1, -2, 2, -3, 3, 4)
N_GATHER, N_SPREAD = 5, 5
SENDS = 40


def dot(left, right):
    return jnp.dot(left, right, preferred_element_type=F32)


def kernel(
    pivot_rhs,
    update_rhs,
    parent_rhs,
    lower_pivot,
    lower_update,
    parent_lower,
    parent_upper,
    upper_pivot,
    upper_update,
    maps,
    parent_out,
    child_out,
    x_pin,
    x_half,
    x_sol,
    x_sum,
    x_mid,
    a_low,
    a_par,
    a_piv,
    a_up,
    cross,
    u_half,
    moved,
    given,
    pick,
    acc,
    direct,
    g_send,
    g_recv,
    s_send,
    s_recv,
    e_send,
    e_recv,
    h_send,
    h_recv,
):
    me_p, me_r = lax.axis_index("panel"), lax.axis_index("rhs")
    core = lax.rem(me_p, 2)
    c = me_p // 2
    z, y_lo = lax.rem(c, Z), c // Z
    x, y_hi = me_r // 4, lax.rem(me_r, 4)
    mate_y = 1 - y_lo
    mate_c = mate_y * Z + z
    sib = me_p + 1 - 2 * core

    def chip(y, dist):
        return y * Z + lax.rem(z + dist + Z, Z)

    def at_z(dist):
        return chip(y_lo, dist) * 2 + core

    def at_xy(dx, dy):
        return lax.rem(x + dx + 4, 4) * 4 + lax.rem(y_hi + dy + 4, 4)

    across = mate_c * 2 + core
    goal = lax.rem(me_p, 2 * Z) * 2

    barrier = pltpu.get_barrier_semaphore()
    friends = [(at_z(d), me_r) for d in (-1, 1, -2, 2)] + [(across, me_r), (sib, me_r)]
    friends += [(me_p, at_xy(*d)) for d in ((0, -1), (0, 1), (-1, 0), (1, 0))]
    for friend in friends:
        pl.semaphore_signal(barrier, inc=1, device_id=friend, device_id_type=MESH)
    for child in range(2):
        source = c + 2 * Z * child

        @pl.when(source != me_p)
        def _():
            pl.semaphore_signal(barrier, inc=1, device_id=(source, me_r), device_id_type=MESH)

    pending = []

    def rcopy(src, dst, send, recv, device):
        return pltpu.make_async_remote_copy(
            src_ref=src, dst_ref=dst, send_sem=send, recv_sem=recv, device_id=device, device_id_type=MESH
        )

    def send(src, dst, ssem, rsem, device, when=None):
        def go():
            rcopy(src, dst, ssem, rsem, device).start()

        def done():
            rcopy(src, dst, ssem, rsem, device).wait_send()

        pending.append((when, done))
        if when is None:
            go()
        else:
            pl.when(when)(go)

    def landed(ref, sem):
        pltpu.make_async_copy(ref, ref, sem).wait()

    class Gather:
        def __init__(self, g, place, kind, cross=None):
            self.g, self.place, self.kind, self.cross, self.n = g, place, kind, cross, 0

        def sem(self, side, col, dist):
            return g_recv.at[self.g, side * 16 + col * 8 + DIST.index(dist)]

        def block(self, col, dist, side=0):
            y = y_lo if col == 0 else mate_y
            return self.place(chip(y, dist), core if side == 0 else 1 - core)

        def put(self, col, dist, to, side, col_there, dist_there, when=None, src=None):
            ref = self.block(col, dist)
            send(
                ref if src is None else src,
                ref,
                g_send.at[self.g, self.n],
                self.sem(side, col_there, dist_there),
                (to, me_r),
                when,
            )
            self.n += 1

        def along(self, col, when=None):
            for d in (2, -2, 1, -1):
                self.put(col, 0, at_z(d), 0, col, -d, when)

        def relay(self, col, d, up, down, when=None):
            if d == -2:
                self.put(col, d, at_z(1), 0, col, -3, when)
                self.put(col, d, at_z(2), 0, col, 4, up)
            if d == 2:
                self.put(col, d, at_z(-1), 0, col, 3, when)
                self.put(col, d, at_z(-2), 0, col, 4, down)

        def start(self):
            if self.kind == "first":
                self.put(0, 0, across, 0, 1, 0, src=self.cross)
            self.along(0)
            if self.kind == "full":
                self.put(0, 0, across, 0, 1, 0)
            self.put(0, 0, sib, 1, 0, 0)

        def hop(self, d):
            landed(self.block(0, d), self.sem(0, 0, d))
            self.relay(0, d, core == 0, core == 1)
            if self.kind == "full":
                self.put(0, d, across, 0, 1, d, core == 0)
            self.put(0, d, sib, 1, 0, d)

        def over(self, d):
            landed(self.block(1, d), self.sem(0, 1, d))
            if self.kind == "first":
                if d == 0:
                    self.along(1)
                self.relay(1, d, core == 0, core == 1)
            else:
                late = core == 1
                even = lax.rem(z, 2) == 0
                if d == 0:
                    self.along(1, late)
                self.relay(
                    1, d, jnp.logical_and(late, even), jnp.logical_and(late, jnp.logical_not(even)), late
                )
            self.put(1, d, sib, 1, 1, d)

        def arrive(self, col, d):
            landed(self.block(col, d, 1), self.sem(1, col, d))

        def near(self):
            if self.kind != "line":
                self.over(0)
            for d in (-2, 2, -1, 1):
                self.hop(d)

        def far(self):
            for d in (-3, 3, 4):
                self.hop(d)
            if self.kind != "line":
                for d in (-2, 2, -1, 1, -3, 3, 4):
                    self.over(d)

        def all_in(self):
            for col in range(1 if self.kind == "line" else 2):
                for d in DIST:
                    self.arrive(col, d)

    class Spread:
        def __init__(self, a, place):
            self.a, self.place, self.n = a, place, 0

        def sem(self, hop, piece):
            return s_recv.at[self.a, hop * 4 + piece]

        def block(self, hop, piece):
            dx = {0: 0, 1: -1, 2: 1, 3: 2}[hop]
            dy = {0: 0, 1: -1, 2: 1, 3: 2}[piece]
            return self.place(at_xy(dx, dy))

        def put(self, hop, piece, to, hop_there, piece_there, when=None):
            ref = self.block(hop, piece)
            send(
                ref,
                ref,
                s_send.at[self.a, self.n],
                self.sem(hop_there, piece_there),
                (me_p, to),
                when,
            )
            self.n += 1

        def start(self):
            self.put(0, 0, at_xy(0, 1), 0, 1)
            self.put(0, 0, at_xy(0, -1), 0, 2)

        def wait(self, hop, piece):
            landed(self.block(hop, piece), self.sem(hop, piece))

        def turn(self):
            self.wait(0, 1)
            self.put(0, 1, at_xy(0, 1), 0, 3, core == 0)
            self.wait(0, 2)
            self.put(0, 2, at_xy(0, -1), 0, 3, core == 1)

        def out(self, piece):
            if piece == 3:
                self.wait(0, 3)
            self.put(0, piece, at_xy(1, 0), 1, piece)
            self.put(0, piece, at_xy(-1, 0), 2, piece)

        def on(self, piece):
            self.wait(1, piece)
            self.put(1, piece, at_xy(1, 0), 3, piece, core == 0)
            self.wait(2, piece)
            self.put(2, piece, at_xy(-1, 0), 3, piece, core == 1)

        def end(self):
            for piece in range(4):
                self.wait(3, piece)

    class Extra:
        def __init__(self, e, ref, c):
            self.e, self.ref = e, ref
            self.dx = lax.rem(x - c // 4 + 4, 4)
            self.dy = lax.rem(y_hi - lax.rem(c, 4) + 4, 4)
            self.n = 0

        def put(self, to, when):
            send(self.ref, self.ref, e_send.at[self.e, self.n], e_recv.at[self.e], (me_p, to), when)
            self.n += 1

        def wait(self, when):
            @pl.when(when)
            def _():
                landed(self.ref, e_recv.at[self.e])

        def both(self, *conditions):
            return functools.reduce(jnp.logical_and, conditions)

        def start(self):
            source = self.both(self.dx == 0, self.dy == 0)
            self.put(at_xy(0, 1), source)
            self.put(at_xy(0, -1), source)
            self.put(at_xy(1, 0), source)
            self.put(at_xy(-1, 0), source)

        def turn(self):
            low, high = self.both(self.dx == 0, self.dy == 1), self.both(self.dx == 0, self.dy == 3)
            near = self.both(self.dx == 0, lax.rem(self.dy, 2) == 1)
            self.wait(near)
            self.put(at_xy(0, 1), self.both(low, core == 0))
            self.put(at_xy(0, -1), self.both(high, core == 1))
            self.put(at_xy(1, 0), near)
            self.put(at_xy(-1, 0), near)

        def out(self):
            far = self.both(self.dx == 0, self.dy == 2)
            self.wait(far)
            self.put(at_xy(1, 0), far)
            self.put(at_xy(-1, 0), far)

        def on(self):
            self.wait(lax.rem(self.dx, 2) == 1)
            self.put(at_xy(1, 0), self.both(self.dx == 1, core == 0))
            self.put(at_xy(-1, 0), self.both(self.dx == 3, core == 1))

        def end(self):
            self.wait(self.dx == 2)

    def slot(r, c=c):
        return r + (r + 15 - c) // 16

    owner = [z, Z + z]

    g_pin = Gather(0, lambda chip_at, core_at: x_pin.at[chip_at, core_at], "first", cross)
    g_sum = Gather(1, lambda chip_at, core_at: x_sum.at[chip_at, core_at], "full")
    g_mid = Gather(2, lambda chip_at, core_at: x_mid.at[chip_at, core_at], "full")
    g_sol = Gather(3, lambda chip_at, core_at: x_sol.at[:, chip_at, core_at], "full")
    g_half = Gather(4, lambda chip_at, core_at: x_half.at[:, lax.rem(chip_at, Z), core_at], "line")
    f_low = Spread(0, lambda r: a_low.at[r])
    f_par = Spread(1, lambda r: a_par.at[slot(r)])
    f_piv = [Spread(2 + j, lambda r, j=j: a_piv.at[j, slot(r, owner[j])]) for j in range(2)]
    f_up = Spread(4, lambda r: a_up.at[r])
    e_par = Extra(0, a_par.at[c + 1], c)
    e_piv = [Extra(1 + j, a_piv.at[j, owner[j] + 1], owner[j]) for j in range(2)]

    x_pin[c, core] = pivot_rhs[y_lo].astype(BF)
    cross[...] = pivot_rhs[mate_y].astype(BF)
    a_low[me_r] = lower_update[...]
    alone = (31 - me_p) // 31 + me_p // 31
    pl.semaphore_wait(barrier, len(friends) + 2 - alone)

    f_low.start()
    g_pin.start()
    f_low.out(0)

    is_low, is_high = me_r <= c, me_r >= c

    @pl.when(is_low)
    def _():
        a_par[me_r] = parent_lower[...]
        a_piv[y_lo, me_r] = lower_pivot[y_lo]

    @pl.when(is_high)
    def _():
        a_par[me_r + 1] = parent_upper[...]
        a_piv[y_lo, me_r + 1] = upper_pivot[y_lo]

    a_up[me_r] = upper_update[...]
    send(
        lower_pivot.at[mate_y],
        a_piv.at[y_lo, me_r],
        h_send.at[1, 0],
        h_recv.at[1, 0],
        (across, me_r),
        is_low,
    )
    send(
        upper_pivot.at[mate_y],
        a_piv.at[y_lo, me_r + 1],
        h_send.at[1, 1],
        h_recv.at[1, 1],
        (across, me_r),
        is_high,
    )

    start = pl.multiple_of(c * 128, 128)
    lanes = [maps[:, pl.ds(k * 2048 + start, 128)] - me_p * 128 for k in range(2)]
    low = jnp.concatenate([lanes[0][:, :64], lanes[1][:, :64]], axis=1)
    high = jnp.concatenate([lanes[0][:, 64:], lanes[1][:, 64:]], axis=1)
    targets = jnp.where(core == 0, low, high)
    rows = lax.broadcasted_iota(jnp.int32, (128, 128), 0)
    chosen = (rows == targets).astype(F32)
    pick[0] = chosen.astype(BF)
    pick[1] = chosen.T.astype(BF)

    g_pin.near()
    f_low.turn()
    f_low.out(1)
    f_low.out(2)
    g_pin.far()
    f_low.out(3)
    f_par.start()
    f_low.on(0)
    f_low.on(1)
    f_low.on(2)
    f_par.out(0)
    g_pin.all_in()
    f_low.on(3)
    f_low.end()

    def square(buffer, r):
        return buffer[r].reshape(128, 128)

    value = update_rhs[...]
    for r in range(16):
        value += dot(a_low[r], square(x_pin, r))
    u_half[...] = value.astype(BF)
    for side in range(2):
        there = goal + side
        piece = u_half.at[pl.ds(side * 64, 64)]
        land = moved.at[y_lo]
        send(piece, land, h_send.at[0, side], h_recv.at[0, y_lo], (there, me_r), there != me_p)

        @pl.when(there == me_p)
        def _():
            pltpu.make_async_copy(piece, land, h_recv.at[0, y_lo]).start()

    f_par.turn()
    f_par.out(1)
    f_par.out(2)
    e_par.start()

    @pl.when(me_r <= mate_c)
    def _():
        ref = a_piv.at[mate_y, me_r]
        landed(ref, h_recv.at[1, 0])

    @pl.when(me_r >= mate_c)
    def _():
        ref = a_piv.at[mate_y, me_r + 1]
        landed(ref, h_recv.at[1, 1])

    for child in range(2):
        landed(moved.at[child], h_recv.at[0, child])
    total = parent_rhs[...] + dot(pick[0], moved[...].reshape(128, 128))
    x_sum[c, core] = total.astype(BF)
    g_sum.start()

    g_sum.near()
    f_par.out(3)
    f_par.on(0)
    f_par.on(1)
    f_par.on(2)
    for j in range(2):
        f_piv[j].start()
        f_piv[j].out(0)
    g_sum.far()
    e_par.turn()
    f_par.on(3)
    g_sum.all_in()
    f_par.end()

    def pair(buffer, r):
        return buffer[r].reshape(256, 128)

    acc[...] = jnp.zeros_like(acc)
    for r in range(16):

        @pl.when(r <= c)
        def _():
            acc[...] += dot(a_par[r], pair(x_sum, r))

    x_mid[c, core] = acc[...].astype(BF)
    g_mid.start()

    for j in range(2):
        f_piv[j].turn()
        f_piv[j].out(1)
        f_piv[j].out(2)
        e_piv[j].start()
    g_mid.near()
    e_par.out()
    for j in range(2):
        f_piv[j].out(3)
        for piece in range(3):
            f_piv[j].on(piece)
    f_up.start()
    f_up.out(0)
    g_mid.far()
    for j in range(2):
        f_piv[j].on(3)
        e_piv[j].turn()
    e_par.on()
    f_up.turn()
    f_up.out(1)
    f_up.out(2)
    g_mid.all_in()
    e_par.end()

    acc[...] = jnp.zeros_like(acc)
    for r in range(16):

        @pl.when(r >= c)
        def _():
            acc[...] += dot(a_par[r + 1], pair(x_mid, r))

    picked = dot(pick[1], acc[...].astype(BF)).astype(BF)
    x_sol[:, c, core] = picked.reshape(2, 64, 128)
    g_sol.start()
    parent_out[...] = acc[...]

    for j in range(2):
        f_piv[j].end()
        e_piv[j].out()
    f_up.out(3)
    direct[...] = jnp.zeros_like(direct)
    for r in range(16):
        for j in range(2):

            @pl.when(r <= owner[j])
            def _():
                direct[j] += dot(a_piv[j, r], square(x_pin, r))

    x_half[:, z, core] = direct[...].astype(BF)
    g_half.start()
    g_sol.near()
    for piece in range(3):
        f_up.on(piece)
    g_half.near()
    g_sol.far()
    for j in range(2):
        e_piv[j].on()
    g_half.far()
    f_up.on(3)
    g_half.all_in()
    for j in range(2):
        e_piv[j].end()

    direct[...] = jnp.zeros_like(direct)
    for r in range(16):
        for j in range(2):

            @pl.when(r >= owner[j])
            def _():
                direct[j] += dot(a_piv[j, r + 1], x_half[r // 8, r % 8].reshape(128, 128))

    send(
        direct.at[mate_y],
        given,
        h_send.at[2, 0],
        h_recv.at[2, 0],
        (across, me_r),
    )
    g_sol.all_in()
    f_up.end()
    for k in range(2):
        value = dot(a_up[0, k], square(x_sol.at[k], 0))
        for r in range(1, 16):
            value += dot(a_up[r, k], square(x_sol.at[k], r))
        child_out[k] = value
    child_out[y_lo] += direct[y_lo]
    landed(given, h_recv.at[2, 0])
    child_out[mate_y] += given[...]

    for when, done in pending:
        if when is None:
            done()
        else:
            pl.when(when)(done)


def shards(*arguments):
    *arrays, maps = arguments
    vm = pltpu.VMEM
    dma = pltpu.SemaphoreType.DMA
    return pl.pallas_call(
        kernel,
        out_shape=(
            jax.ShapeDtypeStruct((128, 128), F32),
            jax.ShapeDtypeStruct((2, 64, 128), F32),
        ),
        in_specs=[pl.BlockSpec(memory_space=pltpu.VMEM)] * 10,
        out_specs=(pl.BlockSpec(memory_space=pltpu.VMEM),) * 2,
        scratch_shapes=[
            vm((16, 2, 64, 128), BF),
            vm((2, Z, 2, 64, 128), BF),
            vm((2, 16, 2, 64, 128), BF),
            vm((16, 2, 128, 128), BF),
            vm((16, 2, 128, 128), BF),
            vm((16, 128, 128), BF),
            vm((17, 128, 256), BF),
            vm((2, 17, 64, 128), BF),
            vm((16, 2, 64, 128), BF),
            vm((64, 128), BF),
            vm((128, 128), BF),
            vm((2, 64, 128), BF),
            vm((64, 128), F32),
            vm((2, 128, 128), BF),
            vm((128, 128), F32),
            vm((2, 64, 128), F32),
            dma((N_GATHER, SENDS)),
            dma((N_GATHER, 32)),
            dma((N_SPREAD, 20)),
            dma((N_SPREAD, 16)),
            dma((3, 12)),
            dma((3,)),
            dma((3, 2)),
            dma((3, 2)),
        ],
        compiler_params=pltpu.CompilerParams(
            collective_id=0, has_side_effects=True, vmem_limit_bytes=60 * 1024 * 1024
        ),
    )(*arrays, maps.reshape(1, -1))


def solution(mesh):
    placed = (
        P(None, "panel", "rhs"),
        P("panel", "rhs"),
        P("panel", "rhs"),
        P(None, "panel", "rhs"),
        P("panel", "rhs"),
        P("panel", "rhs"),
        P("panel", "rhs"),
        P(None, "panel", "rhs"),
        P(None, "panel", "rhs"),
        P(),
    )
    return jax.shard_map(
        shards,
        mesh=mesh,
        in_specs=placed,
        out_specs=(P("panel", "rhs"), P(None, "panel", "rhs")),
        check_vma=False,
    )
```

```python
import functools

import jax
import jax.numpy as jnp
from jax import lax
from jax.experimental import pallas as pl
from jax.experimental.pallas import tpu as pltpu
from jax.sharding import PartitionSpec as P

BF = jnp.bfloat16
F32 = jnp.float32
MESH = pl.DeviceIdType.MESH

Z = 8
DIST = (0, -1, 1, -2, 2, -3, 3, 4)
HOP = {-2: 0, 2: 1, -1: 2, 1: 2, -3: 3, 3: 3, 4: 4}
OVER = {0: 5, -2: 6, 2: 7, -1: 8, 1: 8, -3: 9, 3: 9, 4: 10}
SIBLING = 11
N_GATHER, N_SPREAD, N_EXTRA, N_SEND = 5, 5, 3, 64
RULER = 96


def dot(left, right):
    return jnp.dot(left, right, preferred_element_type=F32)


def kernel(
    pivot_rhs,
    update_rhs,
    parent_rhs,
    lower_pivot,
    lower_update,
    parent_lower,
    parent_upper,
    upper_pivot,
    upper_update,
    maps,
    parent_out,
    child_out,
    x_pin,
    x_half,
    x_sel,
    x_sum,
    x_mid,
    a_low,
    a_par,
    a_piv,
    a_up,
    a_back,
    cross,
    u_half,
    moved,
    given,
    pick,
    direct,
    ruler,
    send_sem,
    g_recv,
    s_recv,
    e_recv,
    h_recv,
):
    me_p, me_r = lax.axis_index("panel"), lax.axis_index("rhs")
    core = lax.rem(me_p, 2)
    c = me_p // 2
    z, y_lo = lax.rem(c, Z), c // Z
    x, y_hi = me_r // 4, lax.rem(me_r, 4)
    mate_y = 1 - y_lo
    mate_c = mate_y * Z + z
    sib = me_p + 1 - 2 * core

    def chip(y, dist):
        return y * Z + lax.rem(z + dist + Z, Z)

    def at_z(dist):
        return chip(y_lo, dist) * 2 + core

    def at_xy(dx, dy):
        return lax.rem(x + dx + 4, 4) * 4 + lax.rem(y_hi + dy + 4, 4)

    across = mate_c * 2 + core
    goal = lax.rem(me_p, 2 * Z) * 2

    barrier = pltpu.get_barrier_semaphore()
    friends = [(at_z(d), me_r) for d in (-1, 1, -2, 2)] + [(across, me_r), (sib, me_r)]
    friends += [(me_p, at_xy(*d)) for d in ((0, -1), (0, 1), (-1, 0), (1, 0))]
    for friend in friends:
        pl.semaphore_signal(barrier, inc=1, device_id=friend, device_id_type=MESH)
    for child in range(2):
        source = c + 2 * Z * child

        @pl.when(source != me_p)
        def _():
            pl.semaphore_signal(barrier, inc=1, device_id=(source, me_r), device_id_type=MESH)

    book = {}

    def send(src, dst, units, recv, device, group, key="all", when=None):
        entry = book.setdefault((group, key), [len(book), 0, when])
        entry[1] += units
        copy = pltpu.make_async_remote_copy(
            src_ref=src,
            dst_ref=dst,
            send_sem=send_sem.at[entry[0]],
            recv_sem=recv,
            device_id=device,
            device_id_type=MESH,
        )
        if when is None:
            copy.start()
        else:
            pl.when(when)(copy.start)

    def landed(units, sem):
        ref = ruler.at[pl.ds(0, units)]
        pltpu.make_async_copy(ref, ref, sem).wait()

    first_core, second_core = core == 0, core == 1
    even = jnp.logical_and(second_core, lax.rem(z, 2) == 0)
    odd = jnp.logical_and(second_core, lax.rem(z, 2) == 1)

    class Gather:
        def __init__(self, g, place, units, kind, cross=None):
            self.g, self.place, self.units, self.kind, self.cross = g, place, units, kind, cross

        def sem(self, side, col, dist):
            spot = SIBLING if side else OVER[dist] if col else HOP[dist]
            return g_recv.at[self.g, spot]

        def block(self, col, dist, side=0):
            y = y_lo if col == 0 else mate_y
            return self.place(chip(y, dist), core if side == 0 else 1 - core)

        def put(self, col, dist, to, side, col_there, dist_there, key="all", when=None, src=None):
            ref = self.block(col, dist)
            send(
                ref if src is None else src,
                ref,
                self.units,
                self.sem(side, col_there, dist_there),
                (to, me_r),
                ("g", self.g),
                key,
                when,
            )

        def along(self, col, key="all", when=None):
            for d in (2, -2, 1, -1):
                self.put(col, 0, at_z(d), 0, col, -d, key, when)

        def relay(self, col, d, up, down, key="all", when=None):
            if d == -2:
                self.put(col, d, at_z(1), 0, col, -3, key, when)
                self.put(col, d, at_z(2), 0, col, 4, *up)
            if d == 2:
                self.put(col, d, at_z(-1), 0, col, 3, key, when)
                self.put(col, d, at_z(-2), 0, col, 4, *down)

        def start(self):
            if self.kind == "first":
                self.put(0, 0, across, 0, 1, 0, src=self.cross)
            self.along(0)
            if self.kind == "full":
                self.put(0, 0, across, 0, 1, 0)
            self.put(0, 0, sib, 1, 0, 0)

        def hop(self, *dists):
            landed(self.units * len(dists), self.sem(0, 0, dists[0]))
            for d in dists:
                self.relay(0, d, ("first", first_core), ("second", second_core))
                if self.kind == "full":
                    self.put(0, d, across, 0, 1, d, "first", first_core)
                self.put(0, d, sib, 1, 0, d)

        def over(self, *dists):
            landed(self.units * len(dists), self.sem(0, 1, dists[0]))
            for d in dists:
                if self.kind == "first":
                    if d == 0:
                        self.along(1)
                    self.relay(1, d, ("first", first_core), ("second", second_core))
                else:
                    if d == 0:
                        self.along(1, "second", second_core)
                    self.relay(1, d, ("even", even), ("odd", odd), "second", second_core)
                self.put(1, d, sib, 1, 1, d)

        def near(self):
            if self.kind != "line":
                self.over(0)
            self.hop(-2)
            self.hop(2)
            self.hop(-1, 1)

        def far(self):
            self.hop(-3, 3)
            self.hop(4)

        def near_over(self):
            self.over(-2)
            self.over(2)
            self.over(-1, 1)

        def far_over(self):
            self.over(-3, 3)
            self.over(4)

        def all_in(self):
            landed(self.units * (8 if self.kind == "line" else 16), self.sem(1, 0, 0))

    class Spread:
        def __init__(self, a, places, units):
            self.a, self.places, self.units = a, places, units

        def sem(self, hop, piece):
            spot = {0: piece - 1, 1: 3 + piece // 3, 2: 5 + piece // 3, 3: 7}[hop]
            return s_recv.at[self.a, spot]

        def put(self, hop, piece, to, hop_there, piece_there, key="all", when=None):
            dx = {0: 0, 1: -1, 2: 1, 3: 2}[hop]
            dy = {0: 0, 1: -1, 2: 1, 3: 2}[piece]
            for place in self.places:
                ref = place(at_xy(dx, dy))
                send(
                    ref,
                    ref,
                    self.units,
                    self.sem(hop_there, piece_there),
                    (me_p, to),
                    ("s", self.a),
                    key,
                    when,
                )

        def start(self):
            self.put(0, 0, at_xy(0, 1), 0, 1)
            self.put(0, 0, at_xy(0, -1), 0, 2)

        def wait(self, hop, piece, count=1):
            landed(self.units * len(self.places) * count, self.sem(hop, piece))

        def turn(self):
            self.wait(0, 1)
            self.put(0, 1, at_xy(0, 1), 0, 3, "first", first_core)
            self.wait(0, 2)
            self.put(0, 2, at_xy(0, -1), 0, 3, "second", second_core)

        def out(self, *pieces):
            for piece in pieces:
                if piece == 3:
                    self.wait(0, 3)
                self.put(0, piece, at_xy(1, 0), 1, piece)
                self.put(0, piece, at_xy(-1, 0), 2, piece)

        def on(self):
            self.wait(1, 0, 3)
            for piece in range(3):
                self.put(1, piece, at_xy(1, 0), 3, piece, "first", first_core)
            self.wait(2, 0, 3)
            for piece in range(3):
                self.put(2, piece, at_xy(-1, 0), 3, piece, "second", second_core)

        def on_last(self):
            self.wait(1, 3)
            self.put(1, 3, at_xy(1, 0), 3, 3, "first", first_core)
            self.wait(2, 3)
            self.put(2, 3, at_xy(-1, 0), 3, 3, "second", second_core)

        def end(self):
            self.wait(3, 0, 4)

    class Extra:
        def __init__(self, e, ref, units, c):
            self.e, self.ref, self.units = e, ref, units
            self.dx = lax.rem(x - c // 4 + 4, 4)
            self.dy = lax.rem(y_hi - lax.rem(c, 4) + 4, 4)

        def put(self, to, key, when):
            send(self.ref, self.ref, self.units, e_recv.at[self.e], (me_p, to), ("e", self.e), key, when)

        def wait(self, when):
            @pl.when(when)
            def _():
                landed(self.units, e_recv.at[self.e])

        def both(self, *conditions):
            return functools.reduce(jnp.logical_and, conditions)

        def start(self):
            source = self.both(self.dx == 0, self.dy == 0)
            for to in ((0, 1), (0, -1), (1, 0), (-1, 0)):
                self.put(at_xy(*to), "source", source)

        def turn(self):
            low, high = self.both(self.dx == 0, self.dy == 1), self.both(self.dx == 0, self.dy == 3)
            near = self.both(self.dx == 0, lax.rem(self.dy, 2) == 1)
            self.wait(near)
            self.put(at_xy(0, 1), "low", self.both(low, first_core))
            self.put(at_xy(0, -1), "high", self.both(high, second_core))
            self.put(at_xy(1, 0), "near", near)
            self.put(at_xy(-1, 0), "near", near)

        def out(self):
            far = self.both(self.dx == 0, self.dy == 2)
            self.wait(far)
            self.put(at_xy(1, 0), "far", far)
            self.put(at_xy(-1, 0), "far", far)

        def on(self):
            self.wait(lax.rem(self.dx, 2) == 1)
            self.put(at_xy(1, 0), "left", self.both(self.dx == 1, first_core))
            self.put(at_xy(-1, 0), "right", self.both(self.dx == 3, second_core))

        def end(self):
            self.wait(self.dx == 2)

    def slot(r, c=c):
        return r + (r + 15 - c) // 16 * 16

    owner = [z, Z + z]

    g_pin = Gather(0, lambda chip_at, core_at: x_pin.at[chip_at, core_at], 1, "first", cross)
    g_sum = Gather(1, lambda chip_at, core_at: x_sum.at[chip_at, core_at], 2, "full")
    g_mid = Gather(2, lambda chip_at, core_at: x_mid.at[chip_at, core_at], 2, "full")
    g_sel = Gather(3, lambda chip_at, core_at: x_sel.at[chip_at, :, core_at], 4, "full")
    g_half = Gather(4, lambda chip_at, core_at: x_half.at[lax.rem(chip_at, Z), core_at], 2, "line")
    f_low = Spread(0, [lambda r: a_low.at[r]], 2)
    f_par = Spread(1, [lambda r: a_par.at[slot(r)]], 4)
    f_piv = Spread(2, [lambda r, j=j: a_piv.at[slot(r, owner[j]), j] for j in range(2)], 1)
    f_up = Spread(3, [lambda r: a_up.at[r]], 2)
    f_back = Spread(4, [lambda r: a_back.at[r]], 4)
    e_par = Extra(0, a_par.at[16 + c], 4, c)
    e_piv = [Extra(1 + j, a_piv.at[16 + owner[j], j], 1, owner[j]) for j in range(2)]
    extras = [e_par] + e_piv

    x_pin[c, core] = pivot_rhs[y_lo].astype(BF)
    cross[...] = pivot_rhs[mate_y].astype(BF)
    a_low[me_r] = lower_update[...]
    alone = (31 - me_p) // 31 + me_p // 31
    pl.semaphore_wait(barrier, len(friends) + 2 - alone)

    f_low.start()
    g_pin.start()
    f_low.out(0)

    is_low, is_high = me_r <= c, me_r >= c
    a_up[me_r] = upper_update[...]
    f_up.start()
    f_up.out(0)

    @pl.when(is_low)
    def _():
        a_par[me_r] = parent_lower[...]
        a_piv[me_r, y_lo] = lower_pivot[y_lo]

    @pl.when(is_high)
    def _():
        a_par[16 + me_r] = parent_upper[...]
        a_piv[16 + me_r, y_lo] = upper_pivot[y_lo]

    @pl.loop(0, 16)
    def _(r):
        @pl.when(r > c)
        def _():
            a_par[r] = jnp.zeros((128, 256), BF)

        @pl.when(r < c)
        def _():
            a_par[16 + r] = jnp.zeros((128, 256), BF)

        for j in range(2):

            @pl.when(r > owner[j])
            def _():
                a_piv[r, j] = jnp.zeros((64, 128), BF)

            @pl.when(r < owner[j])
            def _():
                a_piv[16 + r, j] = jnp.zeros((64, 128), BF)

    def swap(src, dst, spot, when):
        send(src, dst, 1, h_recv.at[spot], (across, me_r), ("swap", spot), "on", when)

    swap(lower_pivot.at[mate_y], a_piv.at[me_r, y_lo], 2, is_low)
    swap(upper_pivot.at[mate_y], a_piv.at[16 + me_r, y_lo], 3, is_high)

    start = pl.multiple_of(c * 128, 128)
    lanes = [maps[:, pl.ds(k * 2048 + start, 128)] - me_p * 128 for k in range(2)]
    low = jnp.concatenate([lanes[0][:, :64], lanes[1][:, :64]], axis=1)
    high = jnp.concatenate([lanes[0][:, 64:], lanes[1][:, 64:]], axis=1)
    targets = jnp.where(core == 0, low, high)
    rows = lax.broadcasted_iota(jnp.int32, (128, 128), 0)
    chosen = (rows == targets).astype(F32)
    pick[...] = chosen.astype(BF)
    x_sel[c, :, core] = dot(chosen.T.astype(BF), parent_upper[...]).astype(BF).reshape(2, 64, 256)

    g_pin.near()
    f_low.turn()
    f_low.out(1, 2)
    g_pin.far()
    g_pin.near_over()
    f_low.out(3)
    f_low.on()
    f_up.turn()
    f_up.out(1, 2)
    g_sel.start()
    g_pin.far_over()
    f_low.on_last()
    g_pin.all_in()
    f_low.end()

    def square(buffer, r):
        return buffer[r].reshape(128, 128)

    def pair(buffer, r):
        return buffer[r].reshape(256, 128)

    def gemm(value, left, right):
        for r in range(16):
            value += dot(left(r), right(r))
        return value

    value = gemm(update_rhs[...], lambda r: a_low[r], lambda r: square(x_pin, r))
    u_half[...] = value.astype(BF)
    for side in range(2):
        there = goal + side
        piece = u_half.at[pl.ds(side * 64, 64)]
        land = moved.at[y_lo]
        send(piece, land, 1, h_recv.at[y_lo], (there, me_r), ("move", side), "on", there != me_p)

        @pl.when(there == me_p)
        def _():
            pltpu.make_async_copy(piece, land, h_recv.at[y_lo]).start()

    g_sel.near()
    f_up.out(3)

    @pl.when(me_r <= mate_c)
    def _():
        landed(1, h_recv.at[2])

    @pl.when(me_r >= mate_c)
    def _():
        landed(1, h_recv.at[3])

    f_piv.start()
    f_piv.out(0)
    f_par.start()
    f_par.out(0)
    for k in range(2):
        landed(1, h_recv.at[k])

    total = parent_rhs[...] + dot(pick[...], moved[...].reshape(128, 128))
    x_sum[c, core] = total.astype(BF)
    g_sum.start()
    g_sel.far()
    f_up.on()
    f_piv.turn()
    f_piv.out(1, 2)
    g_sum.near()
    f_par.turn()
    f_par.out(1, 2)
    f_piv.out(3)
    f_up.on_last()
    g_sel.near_over()
    g_sum.far()
    f_par.out(3)
    f_piv.on()
    g_sel.far_over()
    for extra in extras:
        extra.start()
    g_sum.near_over()
    f_piv.on_last()
    f_par.on()

    g_sel.all_in()
    f_up.end()
    for k in range(2):
        value = gemm(
            jnp.zeros((64, 256), F32), lambda r: a_up[r, k], lambda r: x_sel[r, k].reshape(128, 256)
        )
        a_back[me_r, k * 64 : k * 64 + 64] = value.astype(BF)
    f_back.start()
    f_back.out(0)
    g_sum.far_over()
    f_par.on_last()
    f_piv.end()
    g_sum.all_in()
    f_par.end()

    value = gemm(jnp.zeros((128, 128), F32), lambda r: a_par[r], lambda r: pair(x_sum, r))
    x_mid[c, core] = value.astype(BF)
    g_mid.start()

    value = gemm(jnp.zeros((128, 128), F32), lambda r: square(a_piv, r), lambda r: square(x_pin, r))
    x_half[z, core] = value.astype(BF).reshape(2, 64, 128)
    g_half.start()
    for extra in extras:
        extra.turn()
    f_back.turn()
    f_back.out(1, 2)
    g_mid.near()
    g_half.near()
    for extra in extras:
        extra.out()
    f_back.out(3)
    g_mid.far()
    g_half.far()
    f_back.on()
    for extra in extras:
        extra.on()
    g_mid.near_over()
    for extra in extras:
        extra.end()
    g_half.all_in()

    def half_rows(r):
        return jnp.concatenate([x_half[r % Z, i, r // Z] for i in range(2)], axis=0)

    value = gemm(jnp.zeros((128, 128), F32), lambda r: square(a_piv, 16 + r), half_rows)
    direct[...] = value.reshape(2, 64, 128)
    send(direct.at[mate_y], given, 2, h_recv.at[4], (across, me_r), ("swap", 4))
    f_back.on_last()
    g_mid.far_over()
    f_back.end()
    landed(2, h_recv.at[4])
    g_mid.all_in()

    parent_out[...] = gemm(jnp.zeros((128, 128), F32), lambda r: a_par[16 + r], lambda r: pair(x_mid, r))
    value = gemm(jnp.zeros((128, 128), F32), lambda r: a_back[r], lambda r: pair(x_mid, r))
    child_out[...] = value.reshape(2, 64, 128)
    child_out[y_lo] += direct[y_lo]
    child_out[mate_y] += given[...]

    for spot, units, when in book.values():

        def done():
            landed(units, send_sem.at[spot])

        if when is None:
            done()
        else:
            pl.when(when)(done)


def shards(*arguments):
    *arrays, maps = arguments
    vm = pltpu.VMEM
    dma = pltpu.SemaphoreType.DMA
    return pl.pallas_call(
        kernel,
        out_shape=(
            jax.ShapeDtypeStruct((128, 128), F32),
            jax.ShapeDtypeStruct((2, 64, 128), F32),
        ),
        in_specs=[pl.BlockSpec(memory_space=pltpu.VMEM)] * 10,
        out_specs=(pl.BlockSpec(memory_space=pltpu.VMEM),) * 2,
        scratch_shapes=[
            vm((16, 2, 64, 128), BF),
            vm((Z, 2, 2, 64, 128), BF),
            vm((16, 2, 2, 64, 256), BF),
            vm((16, 2, 128, 128), BF),
            vm((16, 2, 128, 128), BF),
            vm((16, 128, 128), BF),
            vm((32, 128, 256), BF),
            vm((32, 2, 64, 128), BF),
            vm((16, 2, 64, 128), BF),
            vm((16, 128, 256), BF),
            vm((64, 128), BF),
            vm((128, 128), BF),
            vm((2, 64, 128), BF),
            vm((64, 128), F32),
            vm((128, 128), BF),
            vm((2, 64, 128), F32),
            vm((RULER, 64, 128), BF),
            dma((N_SEND,)),
            dma((N_GATHER, 12)),
            dma((N_SPREAD, 8)),
            dma((N_EXTRA,)),
            dma((5,)),
        ],
        compiler_params=pltpu.CompilerParams(
            collective_id=0, has_side_effects=True, vmem_limit_bytes=60 * 1024 * 1024
        ),
    )(*arrays, maps.reshape(1, -1))


def solution(mesh):
    placed = (
        P(None, "panel", "rhs"),
        P("panel", "rhs"),
        P("panel", "rhs"),
        P(None, "panel", "rhs"),
        P("panel", "rhs"),
        P("panel", "rhs"),
        P("panel", "rhs"),
        P(None, "panel", "rhs"),
        P(None, "panel", "rhs"),
        P(),
    )
    return jax.shard_map(
        shards,
        mesh=mesh,
        in_specs=placed,
        out_specs=(P("panel", "rhs"), P(None, "panel", "rhs")),
        check_vma=False,
    )
```

```python
import functools

import jax
import jax.numpy as jnp
from jax import lax
from jax.experimental import pallas as pl
from jax.experimental.pallas import tpu as pltpu
from jax.sharding import PartitionSpec as P

BF = jnp.bfloat16
F32 = jnp.float32
MESH = pl.DeviceIdType.MESH

Z = 8
DIST = (0, -1, 1, -2, 2, -3, 3, 4)
HOP = {-2: 0, 2: 1, -1: 2, 1: 2, -3: 3, 3: 3, 4: 4}
OVER = {0: 5, -2: 6, 2: 7, -1: 8, 1: 8, -3: 9, 3: 9, 4: 10}
SIBLING = 11
N_GATHER, N_SPREAD, N_EXTRA, N_SEND = 6, 4, 3, 56
RULER = 96


def dot(left, right):
    return jnp.dot(left, right, preferred_element_type=F32)


def kernel(
    pivot_rhs,
    update_rhs,
    parent_rhs,
    lower_pivot,
    lower_update,
    parent_lower,
    parent_upper,
    upper_pivot,
    upper_update,
    maps,
    parent_out,
    child_out,
    x_pin,
    x_half,
    x_sol,
    x_sum,
    x_rhs,
    x_mid,
    a_low,
    a_par,
    a_piv,
    a_up,
    cross,
    a_sum,
    acc,
    given,
    pick,
    direct,
    pivot_in,
    update_in,
    parent_in,
    lower_piv_in,
    upper_piv_in,
    maps_in,
    ruler,
    load_sem,
    send_sem,
    g_recv,
    s_recv,
    e_recv,
    h_recv,
):
    me_p, me_r = lax.axis_index("panel"), lax.axis_index("rhs")
    core = lax.rem(me_p, 2)
    c = me_p // 2
    z, y_lo = lax.rem(c, Z), c // Z
    x, y_hi = me_r // 4, lax.rem(me_r, 4)
    mate_y = 1 - y_lo
    mate_c = mate_y * Z + z
    sib = me_p + 1 - 2 * core

    def chip(y, dist):
        return y * Z + lax.rem(z + dist + Z, Z)

    def at_z(dist):
        return chip(y_lo, dist) * 2 + core

    def at_xy(dx, dy):
        return lax.rem(x + dx + 4, 4) * 4 + lax.rem(y_hi + dy + 4, 4)

    def beside(dist):
        return chip(mate_y, dist) * 2 + core

    across = mate_c * 2 + core

    barrier = pltpu.get_barrier_semaphore()
    friends = [(at_z(d), me_r) for d in (-1, 1, -2, 2)] + [(across, me_r), (sib, me_r)]
    friends += [(beside(d), me_r) for d in (-1, 1, -2, 2)]
    friends += [(me_p, at_xy(*d)) for d in ((0, -1), (0, 1), (-1, 0), (1, 0), (0, 2), (2, 0))]
    for friend in friends:
        pl.semaphore_signal(barrier, inc=1, device_id=friend, device_id_type=MESH)
    is_low, is_high = me_r <= c, me_r >= c

    def load(src, dst, spot):
        pltpu.make_async_copy(src, dst, load_sem.at[spot]).start()

    load(lower_update, a_low.at[me_r], 0)
    load(pivot_rhs, pivot_in, 1)
    load(maps, maps_in, 2)
    load(upper_update, a_up.at[me_r], 2)
    load(lower_pivot, lower_piv_in, 2)
    load(upper_pivot, upper_piv_in, 2)
    load(update_rhs, update_in, 2)
    load(parent_rhs, parent_in, 2)

    @pl.when(is_low)
    def _():
        load(parent_lower, a_par.at[me_r], 3)

    @pl.when(is_high)
    def _():
        load(parent_upper, a_par.at[16 + me_r], 4)

    book = {}

    def send(src, dst, units, recv, device, group, key="all", when=None):
        entry = book.setdefault((group, key), [len(book), 0, when])
        entry[1] += units
        copy = pltpu.make_async_remote_copy(
            src_ref=src,
            dst_ref=dst,
            send_sem=send_sem.at[entry[0]],
            recv_sem=recv,
            device_id=device,
            device_id_type=MESH,
        )
        if when is None:
            copy.start()
        else:
            pl.when(when)(copy.start)

    def landed(units, sem):
        ref = ruler.at[pl.ds(0, units)]
        pltpu.make_async_copy(ref, ref, sem).wait()

    first_core, second_core = core == 0, core == 1
    even = jnp.logical_and(second_core, lax.rem(z, 2) == 0)
    odd = jnp.logical_and(second_core, lax.rem(z, 2) == 1)

    class Gather:
        def __init__(self, g, place, units, kind, cross=None):
            self.g, self.place, self.units, self.kind, self.cross = g, place, units, kind, cross

        def sem(self, side, col, dist):
            spot = SIBLING if side else OVER[dist] if col else HOP[dist]
            return g_recv.at[self.g, spot]

        def block(self, col, dist, side=0):
            y = y_lo if col == 0 else mate_y
            return self.place(chip(y, dist), core if side == 0 else 1 - core)

        def put(self, col, dist, to, side, col_there, dist_there, key="all", when=None, src=None):
            ref = self.block(col, dist)
            send(
                ref if src is None else src,
                ref,
                self.units,
                self.sem(side, col_there, dist_there),
                (to, me_r),
                ("g", self.g),
                key,
                when,
            )

        def along(self, col, key="all", when=None):
            for d in (2, -2, 1, -1):
                self.put(col, 0, at_z(d), 0, col, -d, key, when)

        def relay(self, col, d, up, down, key="all", when=None):
            if d == -2:
                self.put(col, d, at_z(1), 0, col, -3, key, when)
                self.put(col, d, at_z(2), 0, col, 4, *up)
            if d == 2:
                self.put(col, d, at_z(-1), 0, col, 3, key, when)
                self.put(col, d, at_z(-2), 0, col, 4, *down)

        def start(self):
            if self.kind == "both":
                for d in (2, -2):
                    self.put(0, 0, at_z(d), 0, 0, -d)
                    self.put(0, 0, beside(d), 0, 1, -d, src=self.cross)
                for d in (1, -1):
                    self.put(0, 0, at_z(d), 0, 0, -d)
                    if self.cross is not None:
                        self.put(0, 0, beside(d), 0, 1, -d, src=self.cross)
            else:
                self.along(0)
            if self.kind != "line":
                self.put(0, 0, across, 0, 1, 0, src=self.cross)
            self.put(0, 0, sib, 1, 0, 0)

        def hop(self, *dists):
            landed(self.units * len(dists), self.sem(0, 0, dists[0]))
            for d in dists:
                self.relay(0, d, ("first", first_core), ("second", second_core))
                if self.kind == "full":
                    self.put(0, d, across, 0, 1, d, "first", first_core)
                if self.kind == "both" and self.cross is None and d in (-1, 1):
                    self.put(0, d, across, 0, 1, d)
                self.put(0, d, sib, 1, 0, d)

        def over(self, *dists):
            landed(self.units * len(dists), self.sem(0, 1, dists[0]))
            for d in dists:
                if self.kind == "both":
                    self.relay(1, d, ("first", first_core), ("second", second_core))
                else:
                    if d == 0:
                        self.along(1, "second", second_core)
                    self.relay(1, d, ("even", even), ("odd", odd), "second", second_core)
                self.put(1, d, sib, 1, 1, d)

        def near(self):
            if self.kind == "full":
                self.over(0)
            self.hop(-2)
            self.hop(2)
            if self.kind == "both":
                self.over(-2)
                self.over(2)
            self.hop(-1, 1)
            if self.kind == "both":
                self.over(0)
                if self.cross is not None:
                    self.over(-1, 1)

        def far(self):
            if self.kind == "both" and self.cross is None:
                self.over(-1, 1)
            self.hop(-3, 3)
            if self.kind == "both":
                self.over(-3, 3)
            self.hop(4)
            if self.kind == "both":
                self.over(4)

        def near_over(self):
            self.over(-2)
            self.over(2)
            self.over(-1, 1)

        def far_over(self):
            self.over(-3, 3)
            self.over(4)

        def all_in(self):
            landed(self.units * (8 if self.kind == "line" else 16), self.sem(1, 0, 0))

    class Spread:
        def __init__(self, a, places, units, jump=False):
            self.a, self.places, self.units, self.jump = a, places, units, jump

        def sem(self, hop, piece):
            spot = {0: piece - 1, 1: 3 + piece // 3, 2: 5 + piece // 3, 3: 7}[hop]
            return s_recv.at[self.a, spot]

        def put(self, hop, piece, to, hop_there, piece_there, key="all", when=None):
            dx = {0: 0, 1: -1, 2: 1, 3: 2}[hop]
            dy = {0: 0, 1: -1, 2: 1, 3: 2}[piece]
            for place in self.places:
                ref = place(at_xy(dx, dy))
                send(
                    ref,
                    ref,
                    self.units,
                    self.sem(hop_there, piece_there),
                    (me_p, to),
                    ("s", self.a),
                    key,
                    when,
                )

        def start(self):
            self.put(0, 0, at_xy(0, 1), 0, 1)
            self.put(0, 0, at_xy(0, -1), 0, 2)
            if self.jump:
                self.put(0, 0, at_xy(0, 2), 0, 3)

        def wait(self, hop, piece, count=1):
            landed(self.units * len(self.places) * count, self.sem(hop, piece))

        def turn(self):
            self.wait(0, 1)
            if not self.jump:
                self.put(0, 1, at_xy(0, 1), 0, 3, "first", first_core)
            self.wait(0, 2)
            if not self.jump:
                self.put(0, 2, at_xy(0, -1), 0, 3, "second", second_core)

        def out(self, *pieces):
            for piece in pieces:
                if piece == 3:
                    self.wait(0, 3)
                self.put(0, piece, at_xy(1, 0), 1, piece)
                self.put(0, piece, at_xy(-1, 0), 2, piece)
                if self.jump and piece in (0, 3):
                    self.put(0, piece, at_xy(2, 0), 3, piece)

        def on(self):
            self.wait(1, 0, 3)
            for piece in range(1 if self.jump else 0, 3):
                self.put(1, piece, at_xy(1, 0), 3, piece, "first", first_core)
            self.wait(2, 0, 3)
            for piece in range(1 if self.jump else 0, 3):
                self.put(2, piece, at_xy(-1, 0), 3, piece, "second", second_core)

        def on_last(self):
            self.wait(1, 3)
            if not self.jump:
                self.put(1, 3, at_xy(1, 0), 3, 3, "first", first_core)
            self.wait(2, 3)
            if not self.jump:
                self.put(2, 3, at_xy(-1, 0), 3, 3, "second", second_core)

        def end(self):
            self.wait(3, 0, 4)

    class Extra:
        def __init__(self, e, ref, units, c):
            self.e, self.ref, self.units = e, ref, units
            self.dx = lax.rem(x - c // 4 + 4, 4)
            self.dy = lax.rem(y_hi - lax.rem(c, 4) + 4, 4)

        def put(self, to, key, when):
            send(self.ref, self.ref, self.units, e_recv.at[self.e], (me_p, to), ("e", self.e), key, when)

        def wait(self, when):
            @pl.when(when)
            def _():
                landed(self.units, e_recv.at[self.e])

        def both(self, *conditions):
            return functools.reduce(jnp.logical_and, conditions)

        def start(self):
            source = self.both(self.dx == 0, self.dy == 0)
            for to in ((0, 1), (0, -1), (1, 0), (-1, 0)):
                self.put(at_xy(*to), "source", source)

        def turn(self):
            low, high = self.both(self.dx == 0, self.dy == 1), self.both(self.dx == 0, self.dy == 3)
            near = self.both(self.dx == 0, lax.rem(self.dy, 2) == 1)
            self.wait(near)
            self.put(at_xy(0, 1), "low", self.both(low, first_core))
            self.put(at_xy(0, -1), "high", self.both(high, second_core))
            self.put(at_xy(1, 0), "near", near)
            self.put(at_xy(-1, 0), "near", near)

        def out(self):
            far = self.both(self.dx == 0, self.dy == 2)
            self.wait(far)
            self.put(at_xy(1, 0), "far", far)
            self.put(at_xy(-1, 0), "far", far)

        def on(self):
            self.wait(lax.rem(self.dx, 2) == 1)
            self.put(at_xy(1, 0), "left", self.both(self.dx == 1, first_core))
            self.put(at_xy(-1, 0), "right", self.both(self.dx == 3, second_core))

        def end(self):
            self.wait(self.dx == 2)

    def update_block(buffer, panel):
        return buffer.at[lax.rem(panel, 2 * Z), panel // (2 * Z)]

    def slot(r, c=c):
        return r + (r + 15 - c) // 16 * 16

    owner = [z, Z + z]

    g_pin = Gather(0, lambda chip_at, core_at: x_pin.at[chip_at, core_at], 1, "both", cross)
    g_sum = Gather(1, lambda chip_at, core_at: update_block(x_sum, chip_at * 2 + core_at), 2, "both")
    g_rhs = Gather(5, lambda chip_at, core_at: x_rhs.at[chip_at, core_at], 2, "full")
    g_mid = Gather(2, lambda chip_at, core_at: x_mid.at[chip_at, core_at], 2, "both")
    g_sol = Gather(3, lambda chip_at, core_at: x_sol.at[:, chip_at, core_at], 2, "both")
    g_half = Gather(4, lambda chip_at, core_at: x_half.at[lax.rem(chip_at, Z), core_at], 2, "line")
    f_low = Spread(0, [lambda r: a_low.at[r]], 2, jump=True)
    f_par = Spread(1, [lambda r: a_par.at[slot(r)]], 4)
    f_piv = Spread(2, [lambda r, j=j: a_piv.at[slot(r, owner[j]), j] for j in range(2)], 1)
    f_up = Spread(3, [lambda r: a_up.at[r]], 2)
    e_par = Extra(0, a_par.at[16 + c], 4, c)
    e_piv = [Extra(1 + j, a_piv.at[16 + owner[j], j], 1, owner[j]) for j in range(2)]
    extras = [e_par] + e_piv

    landed(4, load_sem.at[1])
    x_pin[c, core] = pivot_in[y_lo].astype(BF)
    cross[...] = pivot_in[mate_y].astype(BF)
    landed(2, load_sem.at[0])
    pl.semaphore_wait(barrier, len(friends))

    f_low.start()
    g_pin.start()
    f_low.out(0)

    landed(15, load_sem.at[2])

    @pl.when(is_low)
    def _():
        landed(4, load_sem.at[3])
        a_piv[me_r, y_lo] = lower_piv_in[y_lo]

    @pl.when(is_high)
    def _():
        landed(4, load_sem.at[4])
        a_piv[16 + me_r, y_lo] = upper_piv_in[y_lo]

    @pl.loop(0, 16)
    def _(r):
        @pl.when(r > c)
        def _():
            a_par[r] = jnp.zeros((128, 256), BF)

        @pl.when(r < c)
        def _():
            a_par[16 + r] = jnp.zeros((128, 256), BF)

        for j in range(2):

            @pl.when(r > owner[j])
            def _():
                a_piv[r, j] = jnp.zeros((64, 128), BF)

            @pl.when(r < owner[j])
            def _():
                a_piv[16 + r, j] = jnp.zeros((64, 128), BF)

    def swap(src, dst, spot, when):
        send(src, dst, 1, h_recv.at[spot], (across, me_r), ("swap", spot), "on", when)

    swap(lower_piv_in.at[mate_y], a_piv.at[me_r, y_lo], 2, is_low)
    swap(upper_piv_in.at[mate_y], a_piv.at[16 + me_r, y_lo], 3, is_high)

    start = pl.multiple_of(c * 128, 128)
    lanes = [maps_in[:, pl.ds(k * 2048 + start, 128)] - me_p * 128 for k in range(2)]
    low = jnp.concatenate([lanes[0][:, :64], lanes[1][:, :64]], axis=1)
    high = jnp.concatenate([lanes[0][:, 64:], lanes[1][:, 64:]], axis=1)
    targets = jnp.where(core == 0, low, high)
    rows = lax.broadcasted_iota(jnp.int32, (128, 128), 0)
    chosen = (rows == targets).astype(F32)
    pick[...] = chosen.T.astype(BF)
    x_rhs[c, core] = parent_in[...].astype(BF)

    def square(buffer, r):
        return buffer[r].reshape(128, 128)

    def pair(buffer, r):
        return buffer[r].reshape(256, 128)

    def gemm(value, left, right):
        for r in range(16):
            value += dot(left(r), right(r))
        return value

    g_pin.hop(-2)
    g_pin.hop(2)
    f_low.turn()
    f_low.out(1,2)
    g_pin.over(-2)
    g_pin.over(2)
    f_low.out(3)
    f_par.start()
    g_rhs.start()
    g_pin.hop(-1,1)
    g_pin.over(0)
    g_pin.over(-1,1)
    f_low.on()
    g_pin.far()
    f_low.on_last()
    f_par.out(0)
    f_par.turn()
    f_par.out(1,2)

    @pl.when(me_r <= mate_c)
    def _():
        landed(1, h_recv.at[2])

    @pl.when(me_r >= mate_c)
    def _():
        landed(1, h_recv.at[3])

    f_piv.start()
    g_pin.all_in()
    f_low.end()
    value = gemm(update_in[...], lambda r: a_low[r], lambda r: square(x_pin, r))
    update_block(x_sum, me_p)[...] = value.astype(BF)
    g_sum.start()
    g_rhs.near()
    f_par.out(3)
    f_par.on()
    f_piv.turn()
    f_piv.out(0,1,2)
    for extra in extras:
        extra.start()
    g_sum.near()
    g_rhs.near_over()
    g_rhs.far()
    f_par.on_last()
    f_piv.out(3)
    for extra in extras:
        extra.turn()
    g_sum.far()
    g_rhs.far_over()
    f_piv.on()
    f_up.start()
    f_par.end()
    wide = lax.broadcasted_iota(jnp.int32, (256, 128), 0)
    for r in range(16):
        for k in range(2):
            spot = k * 2048 + r * 128
            chosen = (wide == maps_in[:, spot : spot + 128] - r * 256).astype(F32).astype(BF)
            a_sum[r, :, k * 128 : k * 128 + 128] = dot(a_par[r], chosen).astype(BF)
    g_rhs.all_in()
    acc[...] = gemm(jnp.zeros((128, 128), F32), lambda r: a_par[r], lambda r: pair(x_rhs, r))
    g_sum.all_in()
    value = gemm(acc[...], lambda r: a_sum[r], lambda r: pair(x_sum, r))
    x_mid[c, core] = value.astype(BF)
    g_mid.start()
    for extra in extras:
        extra.out()
    f_piv.on_last()
    f_piv.end()
    value = gemm(jnp.zeros((128, 128), F32), lambda r: square(a_piv, r), lambda r: square(x_pin, r))
    x_half[z, core] = value.astype(BF).reshape(2, 64, 128)
    g_half.start()
    f_up.out(0)
    f_up.turn()
    f_up.out(1,2)
    g_mid.near()
    for extra in extras:
        extra.on()
    g_half.near()
    f_up.out(3)
    g_mid.far()
    for extra in extras:
        extra.end()
    g_half.far()
    f_up.on()
    g_mid.all_in()
    value = gemm(jnp.zeros((128, 128), F32), lambda r: a_par[16 + r], lambda r: pair(x_mid, r))
    x_sol[:, c, core] = dot(pick[...], value.astype(BF)).astype(BF).reshape(2, 64, 128)
    g_sol.start()
    parent_out[...] = value
    g_half.all_in()

    def half_rows(r):
        return jnp.concatenate([x_half[r % Z, i, r // Z] for i in range(2)], axis=0)

    value = gemm(jnp.zeros((128, 128), F32), lambda r: square(a_piv, 16 + r), half_rows)
    direct[...] = value.reshape(2, 64, 128)
    send(direct.at[mate_y], given, 2, h_recv.at[4], (across, me_r), ("swap", 4))
    f_up.on_last()
    g_sol.near()
    g_sol.far()
    landed(2, h_recv.at[4])
    f_up.end()
    child_out[y_lo] = direct[y_lo]
    child_out[mate_y] = given[...]
    g_sol.all_in()
    for k in range(2):
        child_out[k] = gemm(child_out[k], lambda r: a_up[r, k], lambda r: square(x_sol.at[k], r))


    for spot, units, when in book.values():

        def done():
            landed(units, send_sem.at[spot])

        if when is None:
            done()
        else:
            pl.when(when)(done)


def shards(*arguments):
    *arrays, maps = arguments
    vm = pltpu.VMEM
    dma = pltpu.SemaphoreType.DMA
    return pl.pallas_call(
        kernel,
        out_shape=(
            jax.ShapeDtypeStruct((128, 128), F32),
            jax.ShapeDtypeStruct((2, 64, 128), F32),
        ),
        in_specs=[pl.BlockSpec(memory_space=pltpu.HBM)] * 10,
        out_specs=(pl.BlockSpec(memory_space=pltpu.VMEM),) * 2,
        scratch_shapes=[
            vm((16, 2, 64, 128), BF),
            vm((Z, 2, 2, 64, 128), BF),
            vm((2, 16, 2, 64, 128), BF),
            vm((16, 2, 128, 128), BF),
            vm((16, 2, 128, 128), BF),
            vm((16, 2, 128, 128), BF),
            vm((16, 128, 128), BF),
            vm((32, 128, 256), BF),
            vm((32, 2, 64, 128), BF),
            vm((16, 2, 64, 128), BF),
            vm((64, 128), BF),
            vm((16, 128, 256), BF),
            vm((128, 128), F32),
            vm((64, 128), F32),
            vm((128, 128), BF),
            vm((2, 64, 128), F32),
            vm((2, 64, 128), F32),
            vm((128, 128), F32),
            vm((128, 128), F32),
            vm((2, 64, 128), BF),
            vm((2, 64, 128), BF),
            vm((1, 4096), jnp.int32),
            vm((RULER, 64, 128), BF),
            dma((5,)),
            dma((N_SEND,)),
            dma((N_GATHER, 12)),
            dma((N_SPREAD, 8)),
            dma((N_EXTRA,)),
            dma((5,)),
        ],
        compiler_params=pltpu.CompilerParams(
            collective_id=0, has_side_effects=True, vmem_limit_bytes=60 * 1024 * 1024
        ),
    )(*arrays, maps.reshape(1, -1))


def solution(mesh):
    placed = (
        P(None, "panel", "rhs"),
        P("panel", "rhs"),
        P("panel", "rhs"),
        P(None, "panel", "rhs"),
        P("panel", "rhs"),
        P("panel", "rhs"),
        P("panel", "rhs"),
        P(None, "panel", "rhs"),
        P(None, "panel", "rhs"),
        P(),
    )
    return jax.shard_map(
        shards,
        mesh=mesh,
        in_specs=placed,
        out_specs=(P("panel", "rhs"), P(None, "panel", "rhs")),
        check_vma=False,
    )
```

```python
import functools

import jax
import jax.numpy as jnp
from jax import lax
from jax.experimental import pallas as pl
from jax.experimental.pallas import tpu as pltpu
from jax.sharding import PartitionSpec as P

BF = jnp.bfloat16
F32 = jnp.float32
MESH = pl.DeviceIdType.MESH

Z = 8
DIST = (0, -1, 1, -2, 2, -3, 3, 4)
HOP = {-2: 0, 2: 1, -1: 2, 1: 2, -3: 3, 3: 3, 4: 4}
OVER = {0: 5, -2: 6, 2: 7, -1: 8, 1: 8, -3: 9, 3: 9, 4: 10}
SIBLING = 11
N_GATHER, N_SPREAD, N_EXTRA, N_SEND = 6, 4, 3, 60
RULER = 96


def dot(left, right):
    return jnp.dot(left, right, preferred_element_type=F32)


def kernel(
    pivot_rhs,
    update_rhs,
    parent_rhs,
    lower_pivot,
    lower_update,
    parent_lower,
    parent_upper,
    upper_pivot,
    upper_update,
    maps,
    out,
    x_pin,
    x_half,
    x_sol,
    x_sum,
    x_rhs,
    x_mid,
    a_low,
    a_par,
    a_piv,
    a_up,
    cross,
    a_sum,
    acc,
    given,
    pick,
    direct,
    pivot_in,
    update_in,
    parent_in,
    lower_piv_in,
    upper_piv_in,
    maps_in,
    ruler,
    load_sem,
    send_sem,
    g_recv,
    s_recv,
    e_recv,
    h_recv,
):
    parent_out, child_out = out.at[pl.ds(0, 2)], out.at[pl.ds(2, 2)]
    me_p, me_r = lax.axis_index("panel"), lax.axis_index("rhs")
    core = lax.rem(me_p, 2)
    c = me_p // 2
    z, y_lo = lax.rem(c, Z), c // Z
    x, y_hi = me_r // 4, lax.rem(me_r, 4)
    mate_y = 1 - y_lo
    mate_c = mate_y * Z + z
    sib = me_p + 1 - 2 * core

    def chip(y, dist):
        return y * Z + lax.rem(z + dist + Z, Z)

    def at_z(dist):
        return chip(y_lo, dist) * 2 + core

    def at_xy(dx, dy):
        return lax.rem(x + dx + 4, 4) * 4 + lax.rem(y_hi + dy + 4, 4)

    def beside(dist):
        return chip(mate_y, dist) * 2 + core

    across = mate_c * 2 + core

    barrier = pltpu.get_barrier_semaphore()
    friends = [(at_z(d), me_r) for d in (-1, 1, -2, 2)] + [(across, me_r), (sib, me_r)]
    friends += [(beside(d), me_r) for d in (-1, 1, -2, 2)]
    friends += [(me_p, at_xy(*d)) for d in ((0, -1), (0, 1), (-1, 0), (1, 0), (0, 2), (2, 0))]
    for friend in friends:
        pl.semaphore_signal(barrier, inc=1, device_id=friend, device_id_type=MESH)
    is_low, is_high = me_r <= c, me_r >= c

    def load(src, dst, spot):
        pltpu.make_async_copy(src, dst, load_sem.at[spot]).start()

    load(lower_update, a_low.at[me_r], 0)
    load(pivot_rhs, pivot_in, 1)
    load(maps, maps_in, 2)
    load(upper_update, a_up.at[me_r], 2)
    load(lower_pivot, lower_piv_in, 2)
    load(upper_pivot, upper_piv_in, 2)
    load(update_rhs, update_in, 2)
    load(parent_rhs, parent_in, 2)

    @pl.when(is_low)
    def _():
        load(parent_lower, a_par.at[me_r], 3)

    @pl.when(is_high)
    def _():
        load(parent_upper, a_par.at[16 + me_r], 4)

    book = {}

    def send(src, dst, units, recv, device, group, key="all", when=None):
        entry = book.setdefault((group, key), [len(book), 0, when])
        entry[1] += units
        copy = pltpu.make_async_remote_copy(
            src_ref=src,
            dst_ref=dst,
            send_sem=send_sem.at[entry[0]],
            recv_sem=recv,
            device_id=device,
            device_id_type=MESH,
        )
        if when is None:
            copy.start()
        else:
            pl.when(when)(copy.start)

    def landed(units, sem):
        ref = ruler.at[pl.ds(0, units)]
        pltpu.make_async_copy(ref, ref, sem).wait()

    first_core, second_core = core == 0, core == 1
    even = jnp.logical_and(second_core, lax.rem(z, 2) == 0)
    odd = jnp.logical_and(second_core, lax.rem(z, 2) == 1)

    class Gather:
        def __init__(self, g, place, units, kind, cross=None, down=False):
            self.g, self.place, self.units, self.kind, self.cross = g, place, units, kind, cross
            self.down = down
            self.give = ("give", y_lo == 1) if down else ("all", None)
            self.take = ("take", y_lo == 0) if down else ("all", None)
            both = jnp.logical_and
            low = y_lo == 0
            self.up_take = ("take first", both(low, first_core)) if down else ("first", first_core)
            self.down_take = ("take second", both(low, second_core)) if down else ("second", second_core)

        def only(self, action):
            if self.down:
                pl.when(y_lo == 0)(action)
            else:
                action()

        def sem(self, side, col, dist):
            spot = SIBLING + col if side else OVER[dist] if col else HOP[dist]
            return g_recv.at[self.g, spot]

        def block(self, col, dist, side=0):
            y = y_lo if col == 0 else mate_y
            return self.place(chip(y, dist), core if side == 0 else 1 - core)

        def put(self, col, dist, to, side, col_there, dist_there, key="all", when=None, src=None):
            ref = self.block(col, dist)
            send(
                ref if src is None else src,
                ref,
                self.units,
                self.sem(side, col_there, dist_there),
                (to, me_r),
                ("g", self.g),
                key,
                when,
            )

        def along(self, col, key="all", when=None):
            for d in (2, -2, 1, -1):
                self.put(col, 0, at_z(d), 0, col, -d, key, when)

        def relay(self, col, d, up, down, key="all", when=None):
            if d == -2:
                self.put(col, d, at_z(1), 0, col, -3, key, when)
                self.put(col, d, at_z(2), 0, col, 4, *up)
            if d == 2:
                self.put(col, d, at_z(-1), 0, col, 3, key, when)
                self.put(col, d, at_z(-2), 0, col, 4, *down)

        def start(self):
            if self.kind == "both":
                for d in (2, -2):
                    self.put(0, 0, at_z(d), 0, 0, -d)
                    self.put(0, 0, beside(d), 0, 1, -d, *self.give, src=self.cross)
                for d in (1, -1):
                    self.put(0, 0, at_z(d), 0, 0, -d)
                    if self.cross is not None:
                        self.put(0, 0, beside(d), 0, 1, -d, src=self.cross)
            else:
                self.along(0)
            if self.kind != "line":
                self.put(0, 0, across, 0, 1, 0, *self.give, src=self.cross)
            self.put(0, 0, sib, 1, 0, 0)

        def hop(self, *dists):
            landed(self.units * len(dists), self.sem(0, 0, dists[0]))
            for d in dists:
                self.relay(0, d, ("first", first_core), ("second", second_core))
                if self.kind == "full":
                    self.put(0, d, across, 0, 1, d, "first", first_core)
                if self.kind == "both" and self.cross is None and d in (-1, 1):
                    self.put(0, d, across, 0, 1, d, *self.give)
                self.put(0, d, sib, 1, 0, d)

        def over(self, *dists):
            self.only(lambda: landed(self.units * len(dists), self.sem(0, 1, dists[0])))
            for d in dists:
                if self.kind == "both":
                    self.relay(1, d, self.up_take, self.down_take, *self.take)
                else:
                    if d == 0:
                        self.along(1, "second", second_core)
                    self.relay(1, d, ("even", even), ("odd", odd), "second", second_core)
                self.put(1, d, sib, 1, 1, d, *self.take)

        def near(self):
            if self.kind == "full":
                self.over(0)
            self.hop(-2)
            self.hop(2)
            if self.kind == "both":
                self.over(-2)
                self.over(2)
            self.hop(-1, 1)
            if self.kind == "both":
                self.over(0)
                if self.cross is not None:
                    self.over(-1, 1)

        def far(self):
            if self.kind == "both" and self.cross is None:
                self.over(-1, 1)
            self.hop(-3, 3)
            if self.kind == "both":
                self.over(-3, 3)
            self.hop(4)
            if self.kind == "both":
                self.over(4)

        def near_over(self):
            self.over(-2)
            self.over(2)
            self.over(-1, 1)

        def far_over(self):
            self.over(-3, 3)
            self.over(4)

        def all_in(self):
            landed(self.units * 8, self.sem(1, 0, 0))
            if self.kind != "line":
                self.only(lambda: landed(self.units * 8, self.sem(1, 1, 0)))

    class Spread:
        def __init__(self, a, places, units, jump=False, leap=False):
            self.a, self.places, self.units = a, places, units
            self.jump, self.leap = jump, leap

        def sem(self, hop, piece):
            spot = {0: piece - 1, 1: 3 + piece // 3, 2: 5 + piece // 3, 3: 7}[hop]
            return s_recv.at[self.a, spot]

        def put(self, hop, piece, to, hop_there, piece_there, key="all", when=None):
            dx = {0: 0, 1: -1, 2: 1, 3: 2}[hop]
            dy = {0: 0, 1: -1, 2: 1, 3: 2}[piece]
            for place in self.places:
                ref = place(at_xy(dx, dy))
                send(
                    ref,
                    ref,
                    self.units,
                    self.sem(hop_there, piece_there),
                    (me_p, to),
                    ("s", self.a),
                    key,
                    when,
                )

        def start(self):
            self.put(0, 0, at_xy(0, 1), 0, 1)
            self.put(0, 0, at_xy(0, -1), 0, 2)
            if self.jump:
                self.put(0, 0, at_xy(0, 2), 0, 3)

        def wait(self, hop, piece, count=1):
            landed(self.units * len(self.places) * count, self.sem(hop, piece))

        def turn(self):
            self.wait(0, 1)
            if not self.jump:
                self.put(0, 1, at_xy(0, 1), 0, 3, "first", first_core)
            self.wait(0, 2)
            if not self.jump:
                self.put(0, 2, at_xy(0, -1), 0, 3, "second", second_core)

        def out(self, *pieces):
            for piece in pieces:
                if piece == 3:
                    self.wait(0, 3)
                self.put(0, piece, at_xy(1, 0), 1, piece)
                self.put(0, piece, at_xy(-1, 0), 2, piece)
                if self.leap and piece in (0, 3):
                    self.put(0, piece, at_xy(2, 0), 3, piece)

        def on(self):
            self.wait(1, 0, 3)
            for piece in range(1 if self.leap else 0, 3):
                self.put(1, piece, at_xy(1, 0), 3, piece, "first", first_core)
            self.wait(2, 0, 3)
            for piece in range(1 if self.leap else 0, 3):
                self.put(2, piece, at_xy(-1, 0), 3, piece, "second", second_core)

        def on_last(self):
            self.wait(1, 3)
            if not self.leap:
                self.put(1, 3, at_xy(1, 0), 3, 3, "first", first_core)
            self.wait(2, 3)
            if not self.leap:
                self.put(2, 3, at_xy(-1, 0), 3, 3, "second", second_core)

        def end(self):
            self.wait(3, 0, 4)

    class Extra:
        def __init__(self, e, ref, units, c):
            self.e, self.ref, self.units = e, ref, units
            self.dx = lax.rem(x - c // 4 + 4, 4)
            self.dy = lax.rem(y_hi - lax.rem(c, 4) + 4, 4)

        def put(self, to, key, when):
            send(self.ref, self.ref, self.units, e_recv.at[self.e], (me_p, to), ("e", self.e), key, when)

        def wait(self, when):
            @pl.when(when)
            def _():
                landed(self.units, e_recv.at[self.e])

        def both(self, *conditions):
            return functools.reduce(jnp.logical_and, conditions)

        def start(self):
            source = self.both(self.dx == 0, self.dy == 0)
            for to in ((0, 1), (0, -1), (1, 0), (-1, 0)):
                self.put(at_xy(*to), "source", source)

        def turn(self):
            low, high = self.both(self.dx == 0, self.dy == 1), self.both(self.dx == 0, self.dy == 3)
            near = self.both(self.dx == 0, lax.rem(self.dy, 2) == 1)
            self.wait(near)
            self.put(at_xy(0, 1), "low", self.both(low, first_core))
            self.put(at_xy(0, -1), "high", self.both(high, second_core))
            self.put(at_xy(1, 0), "near", near)
            self.put(at_xy(-1, 0), "near", near)

        def out(self):
            far = self.both(self.dx == 0, self.dy == 2)
            self.wait(far)
            self.put(at_xy(1, 0), "far", far)
            self.put(at_xy(-1, 0), "far", far)

        def on(self):
            self.wait(lax.rem(self.dx, 2) == 1)
            self.put(at_xy(1, 0), "left", self.both(self.dx == 1, first_core))
            self.put(at_xy(-1, 0), "right", self.both(self.dx == 3, second_core))

        def end(self):
            self.wait(self.dx == 2)

    def update_block(buffer, panel):
        return buffer.at[lax.rem(panel, 2 * Z), panel // (2 * Z)]

    def slot(r, c=c):
        return r + (r + 15 - c) // 16 * 16

    owner = [z, Z + z]

    g_pin = Gather(0, lambda chip_at, core_at: x_pin.at[chip_at, core_at], 1, "both", cross)
    g_sum = Gather(1, lambda chip_at, core_at: update_block(x_sum, chip_at * 2 + core_at), 2, "both")
    g_rhs = Gather(5, lambda chip_at, core_at: x_rhs.at[chip_at, core_at], 2, "full")
    g_mid = Gather(2, lambda chip_at, core_at: x_mid.at[chip_at, core_at], 2, "both", down=True)
    g_sol = Gather(3, lambda chip_at, core_at: x_sol.at[:, chip_at, core_at], 2, "both")
    g_half = Gather(4, lambda chip_at, core_at: x_half.at[lax.rem(chip_at, Z), core_at], 2, "line")
    f_low = Spread(0, [lambda r: a_low.at[r]], 2, jump=True, leap=True)
    f_par = Spread(1, [lambda r: a_par.at[slot(r)]], 4)
    f_piv = Spread(2, [lambda r, j=j: a_piv.at[slot(r, owner[j]), j] for j in range(2)], 1)
    f_up = Spread(3, [lambda r: a_up.at[r]], 2)
    e_par = Extra(0, a_par.at[16 + c], 4, c)
    e_piv = [Extra(1 + j, a_piv.at[16 + owner[j], j], 1, owner[j]) for j in range(2)]
    extras = [e_par] + e_piv

    landed(4, load_sem.at[1])
    x_pin[c, core] = pivot_in[y_lo].astype(BF)
    cross[...] = pivot_in[mate_y].astype(BF)
    landed(2, load_sem.at[0])
    pl.semaphore_wait(barrier, len(friends))

    f_low.start()
    g_pin.start()
    f_low.out(0)

    landed(15, load_sem.at[2])

    @pl.when(is_low)
    def _():
        landed(4, load_sem.at[3])
        a_piv[me_r, y_lo] = lower_piv_in[y_lo]

    @pl.when(is_high)
    def _():
        landed(4, load_sem.at[4])
        a_piv[16 + me_r, y_lo] = upper_piv_in[y_lo]

    @pl.when(y_lo == 1)
    def _():
        x_mid[:Z] = jnp.zeros((Z, 2, 128, 128), BF)

    @pl.loop(0, 16)
    def _(r):
        @pl.when(r > c)
        def _():
            a_par[r] = jnp.zeros((128, 256), BF)

        @pl.when(r < c)
        def _():
            a_par[16 + r] = jnp.zeros((128, 256), BF)

        for j in range(2):

            @pl.when(r > owner[j])
            def _():
                a_piv[r, j] = jnp.zeros((64, 128), BF)

            @pl.when(r < owner[j])
            def _():
                a_piv[16 + r, j] = jnp.zeros((64, 128), BF)

    def swap(src, dst, spot, when):
        send(src, dst, 1, h_recv.at[spot], (across, me_r), ("swap", spot), "on", when)

    swap(lower_piv_in.at[mate_y], a_piv.at[me_r, y_lo], 2, is_low)
    swap(upper_piv_in.at[mate_y], a_piv.at[16 + me_r, y_lo], 3, is_high)

    start = pl.multiple_of(c * 128, 128)
    lanes = [maps_in[:, pl.ds(k * 2048 + start, 128)] - me_p * 128 for k in range(2)]
    low = jnp.concatenate([lanes[0][:, :64], lanes[1][:, :64]], axis=1)
    high = jnp.concatenate([lanes[0][:, 64:], lanes[1][:, 64:]], axis=1)
    targets = jnp.where(core == 0, low, high)
    rows = lax.broadcasted_iota(jnp.int32, (128, 128), 0)
    chosen = (rows == targets).astype(F32)
    pick[...] = chosen.T.astype(BF)
    x_rhs[c, core] = parent_in[...].astype(BF)

    def square(buffer, r):
        return buffer[r].reshape(128, 128)

    def pair(buffer, r):
        return buffer[r].reshape(256, 128)

    def gemm(value, left, right):
        for r in range(16):
            value += dot(left(r), right(r))
        return value

    g_pin.hop(-2)
    g_pin.hop(2)
    f_low.turn()
    f_low.out(1,2)
    g_pin.over(-2)
    g_pin.over(2)
    f_low.out(3)
    f_par.start()
    g_rhs.start()
    g_pin.hop(-1,1)
    g_pin.over(0)
    g_pin.over(-1,1)
    f_low.on()
    g_pin.far()
    f_low.on_last()
    f_par.out(0)
    f_par.turn()
    f_par.out(1,2)

    @pl.when(me_r <= mate_c)
    def _():
        landed(1, h_recv.at[2])

    @pl.when(me_r >= mate_c)
    def _():
        landed(1, h_recv.at[3])

    f_piv.start()
    g_pin.all_in()
    f_low.end()
    value = gemm(update_in[...], lambda r: a_low[r], lambda r: square(x_pin, r))
    update_block(x_sum, me_p)[...] = value.astype(BF)
    g_sum.start()
    g_rhs.near()
    f_par.out(3)
    f_par.on()
    f_piv.turn()
    f_piv.out(0,1,2)
    for extra in extras:
        extra.start()
    g_sum.near()
    g_rhs.near_over()
    g_rhs.far()
    f_par.on_last()
    f_piv.out(3)
    for extra in extras:
        extra.turn()
    g_sum.far()
    g_rhs.far_over()
    f_piv.on()
    f_up.start()
    f_par.end()
    wide = lax.broadcasted_iota(jnp.int32, (256, 128), 0)
    for r in range(16):
        for k in range(2):
            spot = k * 2048 + r * 128
            chosen = (wide == maps_in[:, spot : spot + 128] - r * 256).astype(F32).astype(BF)
            a_sum[r, :, k * 128 : k * 128 + 128] = dot(a_par[r], chosen).astype(BF)
    g_rhs.all_in()
    acc[...] = gemm(jnp.zeros((128, 128), F32), lambda r: a_par[r], lambda r: pair(x_rhs, r))
    g_sum.all_in()
    value = gemm(acc[...], lambda r: a_sum[r], lambda r: pair(x_sum, r))
    x_mid[c, core] = value.astype(BF)
    g_mid.start()
    for extra in extras:
        extra.out()
    f_piv.on_last()
    f_piv.end()
    value = gemm(jnp.zeros((128, 128), F32), lambda r: square(a_piv, r), lambda r: square(x_pin, r))
    x_half[z, core] = value.astype(BF).reshape(2, 64, 128)
    g_half.start()
    f_up.out(0)
    f_up.turn()
    f_up.out(1,2)
    g_mid.near()
    for extra in extras:
        extra.on()
    g_half.near()
    f_up.out(3)
    g_mid.far()
    for extra in extras:
        extra.end()
    f_up.on()
    g_mid.all_in()
    value = gemm(jnp.zeros((128, 128), F32), lambda r: a_par[16 + r], lambda r: pair(x_mid, r))
    x_sol[:, c, core] = dot(pick[...], value.astype(BF)).astype(BF).reshape(2, 64, 128)
    g_sol.start()
    parent_out[...] = value.reshape(2, 64, 128)
    g_half.far()
    g_half.all_in()

    def half_rows(r):
        return jnp.concatenate([x_half[r % Z, i, r // Z] for i in range(2)], axis=0)

    value = gemm(jnp.zeros((128, 128), F32), lambda r: square(a_piv, 16 + r), half_rows)
    direct[...] = value.reshape(2, 64, 128)
    send(direct.at[mate_y], given, 2, h_recv.at[4], (across, me_r), ("swap", 4))
    f_up.on_last()
    g_sol.near()
    g_sol.far()
    landed(2, h_recv.at[4])
    f_up.end()
    child_out[y_lo] = direct[y_lo]
    child_out[mate_y] = given[...]
    g_sol.all_in()
    for k in range(2):
        child_out[k] = gemm(child_out[k], lambda r: a_up[r, k], lambda r: square(x_sol.at[k], r))


    for spot, units, when in book.values():

        def done():
            landed(units, send_sem.at[spot])

        if when is None:
            done()
        else:
            pl.when(when)(done)


def shards(*arguments):
    *arrays, maps = arguments
    vm = pltpu.VMEM
    dma = pltpu.SemaphoreType.DMA
    out = pl.pallas_call(
        kernel,
        out_shape=jax.ShapeDtypeStruct((4, 64, 128), F32),
        in_specs=[pl.BlockSpec(memory_space=pltpu.HBM)] * 10,
        out_specs=pl.BlockSpec(memory_space=pltpu.VMEM),
        scratch_shapes=[
            vm((16, 2, 64, 128), BF),
            vm((Z, 2, 2, 64, 128), BF),
            vm((2, 16, 2, 64, 128), BF),
            vm((16, 2, 128, 128), BF),
            vm((16, 2, 128, 128), BF),
            vm((16, 2, 128, 128), BF),
            vm((16, 128, 128), BF),
            vm((32, 128, 256), BF),
            vm((32, 2, 64, 128), BF),
            vm((16, 2, 64, 128), BF),
            vm((64, 128), BF),
            vm((16, 128, 256), BF),
            vm((128, 128), F32),
            vm((64, 128), F32),
            vm((128, 128), BF),
            vm((2, 64, 128), F32),
            vm((2, 64, 128), F32),
            vm((128, 128), F32),
            vm((128, 128), F32),
            vm((2, 64, 128), BF),
            vm((2, 64, 128), BF),
            vm((1, 4096), jnp.int32),
            vm((RULER, 64, 128), BF),
            dma((5,)),
            dma((N_SEND,)),
            dma((N_GATHER, 13)),
            dma((N_SPREAD, 8)),
            dma((N_EXTRA,)),
            dma((5,)),
        ],
        compiler_params=pltpu.CompilerParams(
            collective_id=0, has_side_effects=True, vmem_limit_bytes=60 * 1024 * 1024
        ),
    )(*arrays, maps.reshape(1, -1))
    return out[:2].reshape(128, 128), out[2:]


def solution(mesh):
    placed = (
        P(None, "panel", "rhs"),
        P("panel", "rhs"),
        P("panel", "rhs"),
        P(None, "panel", "rhs"),
        P("panel", "rhs"),
        P("panel", "rhs"),
        P("panel", "rhs"),
        P(None, "panel", "rhs"),
        P(None, "panel", "rhs"),
        P(),
    )
    return jax.shard_map(
        shards,
        mesh=mesh,
        in_specs=placed,
        out_specs=(P("panel", "rhs"), P(None, "panel", "rhs")),
        check_vma=False,
    )
```

```python
import functools

import jax
import jax.numpy as jnp
from jax import lax
from jax.experimental import pallas as pl
from jax.experimental.pallas import tpu as pltpu
from jax.sharding import PartitionSpec as P

BF = jnp.bfloat16
F32 = jnp.float32
MESH = pl.DeviceIdType.MESH

Z = 8
DIST = (0, -1, 1, -2, 2, -3, 3, 4)
HOP = {-2: 0, 2: 1, -1: 2, 1: 2, -3: 3, 3: 3, 4: 4}
OVER = {0: 5, -2: 6, 2: 7, -1: 8, 1: 8, -3: 9, 3: 9, 4: 10}
SIBLING = 11
N_GATHER, N_SPREAD, N_EXTRA, N_SEND = 6, 4, 3, 60
RULER = 96


def dot(left, right):
    return jnp.dot(left, right, preferred_element_type=F32)


def kernel(
    pivot_rhs,
    update_rhs,
    parent_rhs,
    lower_pivot,
    lower_update,
    parent_lower,
    parent_upper,
    upper_pivot,
    upper_update,
    maps,
    out,
    x_pin,
    x_half,
    x_sol,
    x_sum,
    x_rhs,
    x_mid,
    a_low,
    a_par,
    a_piv,
    a_up,
    cross,
    a_sum,
    acc,
    given,
    pick,
    direct,
    pivot_in,
    update_in,
    parent_in,
    lower_piv_in,
    upper_piv_in,
    maps_in,
    ruler,
    load_sem,
    send_sem,
    g_recv,
    s_recv,
    e_recv,
    h_recv,
):
    parent_out, child_out = out.at[pl.ds(0, 2)], out.at[pl.ds(2, 2)]
    me_p, me_r = lax.axis_index("panel"), lax.axis_index("rhs")
    core = lax.rem(me_p, 2)
    c = me_p // 2
    z, y_lo = lax.rem(c, Z), c // Z
    x, y_hi = me_r // 4, lax.rem(me_r, 4)
    mate_y = 1 - y_lo
    mate_c = mate_y * Z + z
    sib = me_p + 1 - 2 * core

    def chip(y, dist):
        return y * Z + lax.rem(z + dist + Z, Z)

    def at_z(dist):
        return chip(y_lo, dist) * 2 + core

    def at_xy(dx, dy):
        return lax.rem(x + dx + 4, 4) * 4 + lax.rem(y_hi + dy + 4, 4)

    def beside(dist):
        return chip(mate_y, dist) * 2 + core

    across = mate_c * 2 + core

    barrier = pltpu.get_barrier_semaphore()
    friends = [(at_z(d), me_r) for d in (-1, 1, -2, 2)] + [(across, me_r), (sib, me_r)]
    friends += [(beside(d), me_r) for d in (-1, 1, -2, 2)]
    friends += [(me_p, at_xy(*d)) for d in ((0, -1), (0, 1), (-1, 0), (1, 0), (0, 2), (2, 0))]
    for friend in friends:
        pl.semaphore_signal(barrier, inc=1, device_id=friend, device_id_type=MESH)
    is_low, is_high = me_r <= c, me_r >= c

    def load(src, dst, spot):
        pltpu.make_async_copy(src, dst, load_sem.at[spot]).start()

    load(lower_update, a_low.at[me_r], 0)
    load(pivot_rhs, pivot_in, 1)
    load(maps, maps_in, 2)
    load(upper_update, a_up.at[me_r], 2)
    load(lower_pivot, lower_piv_in, 2)
    load(upper_pivot, upper_piv_in, 2)
    load(update_rhs, update_in, 2)
    load(parent_rhs, parent_in, 2)

    @pl.when(is_low)
    def _():
        load(parent_lower, a_par.at[me_r], 3)

    @pl.when(is_high)
    def _():
        load(parent_upper, a_par.at[16 + me_r], 4)

    book = {}

    def send(src, dst, units, recv, device, group, key="all", when=None):
        entry = book.setdefault((group, key), [len(book), 0, when])
        entry[1] += units
        copy = pltpu.make_async_remote_copy(
            src_ref=src,
            dst_ref=dst,
            send_sem=send_sem.at[entry[0]],
            recv_sem=recv,
            device_id=device,
            device_id_type=MESH,
        )
        if when is None:
            copy.start()
        else:
            pl.when(when)(copy.start)

    def landed(units, sem):
        ref = ruler.at[pl.ds(0, units)]
        pltpu.make_async_copy(ref, ref, sem).wait()

    first_core, second_core = core == 0, core == 1
    even = jnp.logical_and(second_core, lax.rem(z, 2) == 0)
    odd = jnp.logical_and(second_core, lax.rem(z, 2) == 1)

    class Gather:
        def __init__(self, g, place, units, kind, cross=None, down=False):
            self.g, self.place, self.units, self.kind, self.cross = g, place, units, kind, cross
            self.down = down
            self.give = ("give", y_lo == 1) if down else ("all", None)
            self.take = ("take", y_lo == 0) if down else ("all", None)
            both = jnp.logical_and
            low = y_lo == 0
            self.up_take = ("take first", both(low, first_core)) if down else ("first", first_core)
            self.down_take = ("take second", both(low, second_core)) if down else ("second", second_core)

        def only(self, action):
            if self.down:
                pl.when(y_lo == 0)(action)
            else:
                action()

        def sem(self, side, col, dist):
            spot = SIBLING + col if side else OVER[dist] if col else HOP[dist]
            return g_recv.at[self.g, spot]

        def block(self, col, dist, side=0):
            y = y_lo if col == 0 else mate_y
            return self.place(chip(y, dist), core if side == 0 else 1 - core)

        def put(self, col, dist, to, side, col_there, dist_there, key="all", when=None, src=None):
            ref = self.block(col, dist)
            send(
                ref if src is None else src,
                ref,
                self.units,
                self.sem(side, col_there, dist_there),
                (to, me_r),
                ("g", self.g),
                key,
                when,
            )

        def along(self, col, key="all", when=None):
            for d in (2, -2, 1, -1):
                self.put(col, 0, at_z(d), 0, col, -d, key, when)

        def relay(self, col, d, up, down, key="all", when=None):
            if d == -2:
                self.put(col, d, at_z(2), 0, col, 4, *up)
                self.put(col, d, at_z(1), 0, col, -3, key, when)
            if d == 2:
                self.put(col, d, at_z(-2), 0, col, 4, *down)
                self.put(col, d, at_z(-1), 0, col, 3, key, when)

        def start(self):
            if self.kind == "both":
                for d in (2, -2):
                    self.put(0, 0, at_z(d), 0, 0, -d)
                    self.put(0, 0, beside(d), 0, 1, -d, *self.give, src=self.cross)
                for d in (1, -1):
                    self.put(0, 0, at_z(d), 0, 0, -d)
                    if self.cross is not None:
                        self.put(0, 0, beside(d), 0, 1, -d, src=self.cross)
            else:
                self.along(0)
            if self.kind != "line":
                self.put(0, 0, across, 0, 1, 0, *self.give, src=self.cross)
            self.put(0, 0, sib, 1, 0, 0)

        def hop(self, *dists):
            landed(self.units * len(dists), self.sem(0, 0, dists[0]))
            for d in dists:
                self.relay(0, d, ("first", first_core), ("second", second_core))
                if self.kind == "full":
                    self.put(0, d, across, 0, 1, d, "first", first_core)
                if self.kind == "both" and self.cross is None and d in (-1, 1):
                    self.put(0, d, across, 0, 1, d, *self.give)
                self.put(0, d, sib, 1, 0, d)

        def over(self, *dists):
            self.only(lambda: landed(self.units * len(dists), self.sem(0, 1, dists[0])))
            for d in dists:
                if self.kind == "both":
                    self.relay(1, d, self.up_take, self.down_take, *self.take)
                else:
                    if d == 0:
                        self.along(1, "second", second_core)
                    self.relay(1, d, ("even", even), ("odd", odd), "second", second_core)
                self.put(1, d, sib, 1, 1, d, *self.take)

        def near(self):
            if self.kind == "full":
                self.over(0)
            self.hop(-2)
            self.hop(2)
            if self.kind == "both" and self.cross is None:
                self.hop(-1, 1)
            if self.kind == "both":
                self.over(-2)
                self.over(2)
            if self.kind != "both" or self.cross is not None:
                self.hop(-1, 1)
            if self.kind == "both":
                self.over(0)
                if self.cross is not None:
                    self.over(-1, 1)

        def far(self):
            if self.kind == "both" and self.cross is None:
                self.over(-1, 1)
            self.hop(-3, 3)
            if self.kind == "both":
                self.over(-3, 3)
            self.hop(4)
            if self.kind == "both":
                self.over(4)

        def near_over(self):
            self.over(-2)
            self.over(2)
            self.over(-1, 1)

        def far_over(self):
            self.over(-3, 3)
            self.over(4)

        def all_in(self):
            landed(self.units * 8, self.sem(1, 0, 0))
            if self.kind != "line":
                self.only(lambda: landed(self.units * 8, self.sem(1, 1, 0)))

    class Spread:
        def __init__(self, a, places, units, jump=False, leap=False):
            self.a, self.places, self.units = a, places, units
            self.jump, self.leap = jump, leap

        def sem(self, hop, piece):
            spot = {0: piece - 1, 1: 3 + piece // 3, 2: 5 + piece // 3, 3: 7}[hop]
            return s_recv.at[self.a, spot]

        def put(self, hop, piece, to, hop_there, piece_there, key="all", when=None):
            dx = {0: 0, 1: -1, 2: 1, 3: 2}[hop]
            dy = {0: 0, 1: -1, 2: 1, 3: 2}[piece]
            for place in self.places:
                ref = place(at_xy(dx, dy))
                send(
                    ref,
                    ref,
                    self.units,
                    self.sem(hop_there, piece_there),
                    (me_p, to),
                    ("s", self.a),
                    key,
                    when,
                )

        def start(self):
            self.put(0, 0, at_xy(0, 1), 0, 1)
            self.put(0, 0, at_xy(0, -1), 0, 2)
            if self.jump:
                self.put(0, 0, at_xy(0, 2), 0, 3)

        def wait(self, hop, piece, count=1):
            landed(self.units * len(self.places) * count, self.sem(hop, piece))

        def turn(self):
            self.wait(0, 1)
            if not self.jump:
                self.put(0, 1, at_xy(0, 1), 0, 3, "first", first_core)
            self.wait(0, 2)
            if not self.jump:
                self.put(0, 2, at_xy(0, -1), 0, 3, "second", second_core)

        def out(self, *pieces):
            for piece in pieces:
                if piece == 3:
                    self.wait(0, 3)
                self.put(0, piece, at_xy(1, 0), 1, piece)
                self.put(0, piece, at_xy(-1, 0), 2, piece)
                if self.leap and piece in (0, 3):
                    self.put(0, piece, at_xy(2, 0), 3, piece)

        def on(self):
            self.wait(1, 0, 3)
            for piece in range(1 if self.leap else 0, 3):
                self.put(1, piece, at_xy(1, 0), 3, piece, "first", first_core)
            self.wait(2, 0, 3)
            for piece in range(1 if self.leap else 0, 3):
                self.put(2, piece, at_xy(-1, 0), 3, piece, "second", second_core)

        def on_last(self):
            self.wait(1, 3)
            if not self.leap:
                self.put(1, 3, at_xy(1, 0), 3, 3, "first", first_core)
            self.wait(2, 3)
            if not self.leap:
                self.put(2, 3, at_xy(-1, 0), 3, 3, "second", second_core)

        def end(self):
            self.wait(3, 0, 4)

    class Extra:
        def __init__(self, e, ref, units, c):
            self.e, self.ref, self.units = e, ref, units
            self.dx = lax.rem(x - c // 4 + 4, 4)
            self.dy = lax.rem(y_hi - lax.rem(c, 4) + 4, 4)

        def put(self, to, key, when):
            send(self.ref, self.ref, self.units, e_recv.at[self.e], (me_p, to), ("e", self.e), key, when)

        def wait(self, when):
            @pl.when(when)
            def _():
                landed(self.units, e_recv.at[self.e])

        def both(self, *conditions):
            return functools.reduce(jnp.logical_and, conditions)

        def start(self):
            source = self.both(self.dx == 0, self.dy == 0)
            for to in ((0, 1), (0, -1), (1, 0), (-1, 0)):
                self.put(at_xy(*to), "source", source)

        def turn(self):
            low, high = self.both(self.dx == 0, self.dy == 1), self.both(self.dx == 0, self.dy == 3)
            near = self.both(self.dx == 0, lax.rem(self.dy, 2) == 1)
            self.wait(near)
            self.put(at_xy(0, 1), "low", self.both(low, first_core))
            self.put(at_xy(0, -1), "high", self.both(high, second_core))
            self.put(at_xy(1, 0), "near", near)
            self.put(at_xy(-1, 0), "near", near)

        def out(self):
            far = self.both(self.dx == 0, self.dy == 2)
            self.wait(far)
            self.put(at_xy(1, 0), "far", far)
            self.put(at_xy(-1, 0), "far", far)

        def on(self):
            self.wait(lax.rem(self.dx, 2) == 1)
            self.put(at_xy(1, 0), "left", self.both(self.dx == 1, first_core))
            self.put(at_xy(-1, 0), "right", self.both(self.dx == 3, second_core))

        def end(self):
            self.wait(self.dx == 2)

    def update_block(buffer, panel):
        return buffer.at[lax.rem(panel, 2 * Z), panel // (2 * Z)]

    def slot(r, c=c):
        return r + (r + 15 - c) // 16 * 16

    owner = [z, Z + z]

    g_pin = Gather(0, lambda chip_at, core_at: x_pin.at[chip_at, core_at], 1, "both", cross)
    g_sum = Gather(1, lambda chip_at, core_at: update_block(x_sum, chip_at * 2 + core_at), 2, "both")
    g_rhs = Gather(5, lambda chip_at, core_at: x_rhs.at[chip_at, core_at], 2, "full")
    g_mid = Gather(2, lambda chip_at, core_at: x_mid.at[chip_at, core_at], 2, "both", down=True)
    g_sol = Gather(3, lambda chip_at, core_at: x_sol.at[:, chip_at, core_at], 2, "both")
    g_half = Gather(4, lambda chip_at, core_at: x_half.at[lax.rem(chip_at, Z), core_at], 2, "line")
    f_low = Spread(0, [lambda r: a_low.at[r]], 2, jump=True, leap=True)
    f_par = Spread(1, [lambda r: a_par.at[slot(r)]], 4)
    f_piv = Spread(2, [lambda r, j=j: a_piv.at[slot(r, owner[j]), j] for j in range(2)], 1)
    f_up = Spread(3, [lambda r: a_up.at[r]], 2)
    e_par = Extra(0, a_par.at[16 + c], 4, c)
    e_piv = [Extra(1 + j, a_piv.at[16 + owner[j], j], 1, owner[j]) for j in range(2)]
    extras = [e_par] + e_piv

    landed(4, load_sem.at[1])
    x_pin[c, core] = pivot_in[y_lo].astype(BF)
    cross[...] = pivot_in[mate_y].astype(BF)
    landed(2, load_sem.at[0])
    pl.semaphore_wait(barrier, len(friends))

    f_low.start()
    g_pin.start()
    f_low.out(0)

    landed(15, load_sem.at[2])

    @pl.when(is_low)
    def _():
        landed(4, load_sem.at[3])
        a_piv[me_r, y_lo] = lower_piv_in[y_lo]

    @pl.when(is_high)
    def _():
        landed(4, load_sem.at[4])
        a_piv[16 + me_r, y_lo] = upper_piv_in[y_lo]

    @pl.when(y_lo == 1)
    def _():
        x_mid[:Z] = jnp.zeros((Z, 2, 128, 128), BF)

    @pl.loop(0, 16)
    def _(r):
        @pl.when(r > c)
        def _():
            a_par[r] = jnp.zeros((128, 256), BF)

        @pl.when(r < c)
        def _():
            a_par[16 + r] = jnp.zeros((128, 256), BF)

        for j in range(2):

            @pl.when(r > owner[j])
            def _():
                a_piv[r, j] = jnp.zeros((64, 128), BF)

            @pl.when(r < owner[j])
            def _():
                a_piv[16 + r, j] = jnp.zeros((64, 128), BF)

    def swap(src, dst, spot, when):
        send(src, dst, 1, h_recv.at[spot], (across, me_r), ("swap", spot), "on", when)

    swap(lower_piv_in.at[mate_y], a_piv.at[me_r, y_lo], 2, is_low)
    swap(upper_piv_in.at[mate_y], a_piv.at[16 + me_r, y_lo], 3, is_high)

    start = pl.multiple_of(c * 128, 128)
    lanes = [maps_in[:, pl.ds(k * 2048 + start, 128)] - me_p * 128 for k in range(2)]
    low = jnp.concatenate([lanes[0][:, :64], lanes[1][:, :64]], axis=1)
    high = jnp.concatenate([lanes[0][:, 64:], lanes[1][:, 64:]], axis=1)
    targets = jnp.where(core == 0, low, high)
    rows = lax.broadcasted_iota(jnp.int32, (128, 128), 0)
    chosen = (rows == targets).astype(F32)
    pick[...] = chosen.T.astype(BF)
    x_rhs[c, core] = parent_in[...].astype(BF)

    def square(buffer, r):
        return buffer[r].reshape(128, 128)

    def pair(buffer, r):
        return buffer[r].reshape(256, 128)

    def gemm(value, left, right):
        for r in range(16):
            value += dot(left(r), right(r))
        return value

    g_pin.hop(-2)
    g_pin.hop(2)
    f_low.turn()
    f_low.out(1,2)
    g_pin.over(-2)
    g_pin.over(2)
    f_low.out(3)
    f_par.start()
    g_rhs.start()
    g_pin.hop(-1,1)
    g_pin.over(0)
    g_pin.over(-1,1)
    f_low.on()
    g_pin.far()
    f_low.on_last()
    f_par.out(0)
    f_par.turn()
    f_par.out(1,2)

    @pl.when(me_r <= mate_c)
    def _():
        landed(1, h_recv.at[2])

    @pl.when(me_r >= mate_c)
    def _():
        landed(1, h_recv.at[3])

    f_piv.start()
    g_pin.all_in()
    f_low.end()
    value = gemm(update_in[...], lambda r: a_low[r], lambda r: square(x_pin, r))
    update_block(x_sum, me_p)[...] = value.astype(BF)
    g_sum.start()
    g_rhs.near()
    f_par.out(3)
    f_par.on()
    f_piv.turn()
    f_piv.out(0,1,2)
    for extra in extras:
        extra.start()
    g_sum.near()
    g_rhs.near_over()
    g_rhs.far()
    f_par.on_last()
    f_piv.out(3)
    for extra in extras:
        extra.turn()
    g_rhs.far_over()
    g_sum.far()
    f_piv.on()
    f_up.start()
    f_par.end()
    wide = lax.broadcasted_iota(jnp.int32, (256, 128), 0)
    for r in range(16):
        for k in range(2):
            spot = k * 2048 + r * 128
            chosen = (wide == maps_in[:, spot : spot + 128] - r * 256).astype(F32).astype(BF)
            a_sum[r, :, k * 128 : k * 128 + 128] = dot(a_par[r], chosen).astype(BF)
    g_rhs.all_in()
    acc[...] = gemm(jnp.zeros((128, 128), F32), lambda r: a_par[r], lambda r: pair(x_rhs, r))
    g_sum.all_in()
    value = gemm(acc[...], lambda r: a_sum[r], lambda r: pair(x_sum, r))
    x_mid[c, core] = value.astype(BF)
    g_mid.start()
    for extra in extras:
        extra.out()
    f_piv.on_last()
    f_up.out(0)
    f_up.turn()
    f_up.out(1,2)
    g_mid.near()
    f_piv.end()
    value = gemm(jnp.zeros((128, 128), F32), lambda r: square(a_piv, r), lambda r: square(x_pin, r))
    x_half[z, core] = value.astype(BF).reshape(2, 64, 128)
    g_half.start()
    for extra in extras:
        extra.on()
    f_up.out(3)
    g_mid.far()
    for extra in extras:
        extra.end()
    f_up.on()
    g_mid.all_in()
    value = gemm(jnp.zeros((128, 128), F32), lambda r: a_par[16 + r], lambda r: pair(x_mid, r))
    x_sol[:, c, core] = dot(pick[...], value.astype(BF)).astype(BF).reshape(2, 64, 128)
    g_sol.start()
    parent_out[...] = value.reshape(2, 64, 128)
    g_half.near()
    f_up.on_last()
    g_sol.near()
    g_half.far()
    g_half.all_in()

    def half_rows(r):
        return jnp.concatenate([x_half[r % Z, i, r // Z] for i in range(2)], axis=0)

    value = gemm(jnp.zeros((128, 128), F32), lambda r: square(a_piv, 16 + r), half_rows)
    direct[...] = value.reshape(2, 64, 128)
    send(direct.at[mate_y], given, 2, h_recv.at[4], (across, me_r), ("swap", 4))
    g_sol.far()
    landed(2, h_recv.at[4])
    f_up.end()
    child_out[y_lo] = direct[y_lo]
    child_out[mate_y] = given[...]
    g_sol.all_in()
    for k in range(2):
        child_out[k] = gemm(child_out[k], lambda r: a_up[r, k], lambda r: square(x_sol.at[k], r))


    for spot, units, when in book.values():

        def done():
            landed(units, send_sem.at[spot])

        if when is None:
            done()
        else:
            pl.when(when)(done)


def shards(*arguments):
    *arrays, maps = arguments
    vm = pltpu.VMEM
    dma = pltpu.SemaphoreType.DMA
    out = pl.pallas_call(
        kernel,
        out_shape=jax.ShapeDtypeStruct((4, 64, 128), F32),
        in_specs=[pl.BlockSpec(memory_space=pltpu.HBM)] * 10,
        out_specs=pl.BlockSpec(memory_space=pltpu.VMEM),
        scratch_shapes=[
            vm((16, 2, 64, 128), BF),
            vm((Z, 2, 2, 64, 128), BF),
            vm((2, 16, 2, 64, 128), BF),
            vm((16, 2, 128, 128), BF),
            vm((16, 2, 128, 128), BF),
            vm((16, 2, 128, 128), BF),
            vm((16, 128, 128), BF),
            vm((32, 128, 256), BF),
            vm((32, 2, 64, 128), BF),
            vm((16, 2, 64, 128), BF),
            vm((64, 128), BF),
            vm((16, 128, 256), BF),
            vm((128, 128), F32),
            vm((64, 128), F32),
            vm((128, 128), BF),
            vm((2, 64, 128), F32),
            vm((2, 64, 128), F32),
            vm((128, 128), F32),
            vm((128, 128), F32),
            vm((2, 64, 128), BF),
            vm((2, 64, 128), BF),
            vm((1, 4096), jnp.int32),
            vm((RULER, 64, 128), BF),
            dma((5,)),
            dma((N_SEND,)),
            dma((N_GATHER, 13)),
            dma((N_SPREAD, 8)),
            dma((N_EXTRA,)),
            dma((5,)),
        ],
        compiler_params=pltpu.CompilerParams(
            collective_id=0, has_side_effects=True, vmem_limit_bytes=60 * 1024 * 1024
        ),
    )(*arrays, maps.reshape(1, -1))
    return out[:2].reshape(128, 128), out[2:]


def solution(mesh):
    placed = (
        P(None, "panel", "rhs"),
        P("panel", "rhs"),
        P("panel", "rhs"),
        P(None, "panel", "rhs"),
        P("panel", "rhs"),
        P("panel", "rhs"),
        P("panel", "rhs"),
        P(None, "panel", "rhs"),
        P(None, "panel", "rhs"),
        P(),
    )
    return jax.shard_map(
        shards,
        mesh=mesh,
        in_specs=placed,
        out_specs=(P("panel", "rhs"), P(None, "panel", "rhs")),
        check_vma=False,
    )
```
